32 devices in a mesh: cluster: 8 (over z, y), sub: 4 (over x, core).
Axes of the slice: x: 2, y: 2, z: 4, core: 2. Of those that a mesh axis runs over, the one named last changes fastest.
Arguments:
- rhs: float32 [128, 4, 384], P(('cluster', 'sub')), may hold values from -8 to 8
- operators: bfloat16 [128, 384, 384], P(('cluster', 'sub')), may hold values from -1 to 5
- signs: int32 [128, 384], P(('cluster', 'sub')), may hold values from -1 to 1, as said below
- links: int32 [128, 3, 128], P(('cluster', 'sub')), may hold values from 0 to 127, as said below
- cluster_basis: float32 [128, 24, 384], P(('cluster', 'sub')), may hold values from -0.3125 to 0.3125
- corner_basis: float32 [128, 8, 384], P(('cluster', 'sub')), may hold values from -0.3125 to 0.3125
- corner_ids: int32 [128, 8], P(('cluster', 'sub')), may hold values from 0 to 127
- cluster_coarse: float32 [8, 384, 384], P('cluster', 'sub'), may hold values from -1 to 3
- global_coarse: float32 [128, 128], P('sub'), may hold values from -0.2 to 0.5
Outputs:
- multipliers: float32 [128, 4, 384], P(('cluster', 'sub'))
- residual: float32 [128, 4, 384], P(('cluster', 'sub'))
The draws below stay inside these ranges and needn't reach their ends.
Inputs may be any that keep to these rules, and one draw needn't show every extreme that they name: `signs`: each entry is -1 or 1. Each links[s, b] is a permutation of 0 to 127; both subdomains of an interface pair hold the same permutation for it.
All inputs are finite; a program needn't handle non-finite values.
Results may differ from the reference program's by a relative error of at most 0.007.
Values sent between devices are 32-bit elements; how exact they have to be, the bound alone decides.
A program may use at most 64 MiB of HBM per device.

```python
import math
from functools import partial
import jax
import jax.numpy as jnp
from jax import lax

SUB_DEV = 4
LOADS = 4
BLK = 128
KC = 24
CORN = 8
ITERS = 2
DUAL = 384
CLUSTERS = 8
SUBS = 128
CCO = 384
NG = 128
N_SUB = 4


def draw_rhs(key, part):
    position = jnp.arange(SUBS, dtype=jnp.float32) / SUBS
    values = jnp.clip(jax.random.normal(key, (SUBS, LOADS, DUAL), jnp.float32), -4.0, 4.0)
    scaling = 0.6 + 1.2 * position
    return values * scaling[:, None, None]


def draw_operators(key, part):
    first_key, second_key = jax.random.split(key)
    identity = jnp.eye(DUAL, dtype=jnp.float32)
    diagonal = jnp.exp(jax.random.uniform(first_key, (SUBS, DUAL), jnp.float32, 0.0, math.log(4.0)))
    coupling = jnp.clip(jax.random.normal(second_key, (SUBS, DUAL, DUAL), jnp.float32), -4.0, 4.0) * (0.3 / math.sqrt(DUAL))
    return (coupling * (1.0 - identity) + diagonal[:, :, None] * identity).astype(jnp.bfloat16)


def coarse_matrix(key, leading, order):
    second_key = jax.random.fold_in(key, 1)
    identity = jnp.eye(order, dtype=jnp.float32)
    diagonal = jnp.ones(leading + (order,), jnp.float32)
    coupling = jnp.clip(jax.random.normal(second_key, leading + (order, order), jnp.float32), -4.0, 4.0) * (0.5 / math.sqrt(order))
    return coupling * (1.0 - identity) + diagonal[..., None] * identity


def draw_cluster_coarse(key, part):
    return coarse_matrix(key, (CLUSTERS,), CCO)


def draw_global_coarse(key, part):
    return 0.15 * coarse_matrix(key, (), NG)


def draw_signs(key, part):
    return 2 * jax.random.randint(key, (SUBS, DUAL), 0, 2, jnp.int32) - 1


def shuffle(base_key, pair_id):
    return jax.random.permutation(jax.random.fold_in(base_key, pair_id), BLK)


def draw_links(key, part):
    numbers = jnp.arange(SUBS, dtype=jnp.int32)
    member = numbers % SUB_DEV
    position = numbers // SUB_DEV % N_SUB
    cluster = numbers // (SUB_DEV * N_SUB)
    stride = SUB_DEV * N_SUB
    down_pair = jnp.where(position > 0, numbers - SUB_DEV, numbers + SUBS)
    across_pair = jnp.where(member % 2 == 0, numbers, jnp.where(cluster > 0, numbers - stride - 1, numbers + SUBS))
    inside_key = jax.random.fold_in(key, 11)
    outside_key = jax.random.fold_in(key, 23)
    up_order = jax.vmap(partial(shuffle, inside_key))(numbers)
    down_order = jax.vmap(partial(shuffle, inside_key))(down_pair)
    across_order = jax.vmap(partial(shuffle, outside_key))(across_pair)
    return jnp.stack([up_order, down_order, across_order], axis=1).astype(jnp.int32)


def with_ends(values, stream_key, least, largest):
    index_at = [jax.random.randint(jax.random.fold_in(stream_key, axis), (), 0, length) for axis, length in enumerate(values.shape)]
    widest = values.shape.index(max(values.shape))
    neighbour = index_at[:widest] + [(index_at[widest] + 1) % values.shape[widest]] + index_at[widest + 1:]
    return values.at[tuple(index_at)].set(least).at[tuple(neighbour)].set(largest)


def shard_levels(stream_key, shape, pieces, smallest, largest):
    factor_of = 1.0
    for dim, blocks in pieces:
        draws = jax.random.uniform(jax.random.fold_in(jax.random.fold_in(stream_key, 6), dim), (blocks,), jnp.float32, smallest / len(pieces), largest / len(pieces))
        factor_of = factor_of * jnp.repeat(jnp.exp(draws), shape[dim] // blocks).reshape((-1,) + (1,) * (len(shape) - 1 - dim))
    return factor_of


def scatter_about(key, shape, deviation, most, pieces=(), held_as=jnp.bfloat16):
    entries = jax.random.normal(key, shape, jnp.float32) * deviation
    if len(pieces) > 0:
        entries = shard_levels(key, shape, pieces, -0.22, 0.18) * entries
    return jnp.clip(entries, min=-most, max=most).astype(held_as)


def setup_inputs(seed: int = 0) -> dict:
    streams_of = jax.random.split(jax.random.key(seed), 10)
    rhs = draw_rhs(jax.random.fold_in(streams_of[9], 71), 0)
    operators = draw_operators(jax.random.fold_in(streams_of[9], 71), 0)
    signs = draw_signs(jax.random.fold_in(streams_of[9], 71), 0)
    links = draw_links(jax.random.fold_in(streams_of[9], 71), 0)
    cluster_basis = scatter_about(streams_of[4], (SUBS, KC, DUAL), DUAL ** -0.5, 0.3125, ((0, 32),), jnp.float32)
    corner_basis = scatter_about(streams_of[5], (SUBS, CORN, DUAL), DUAL ** -0.5, 0.3125, ((0, 32),), jnp.float32)
    corner_ids = with_ends(jax.random.randint(streams_of[6], (SUBS, CORN), 0, NG), jax.random.fold_in(streams_of[6], 1), 0, NG - 1).astype(jnp.int32)
    cluster_coarse = draw_cluster_coarse(jax.random.fold_in(streams_of[9], 71), 0)
    global_coarse = draw_global_coarse(jax.random.fold_in(streams_of[9], 71), 0)
    return {"rhs": rhs, "operators": operators, "signs": signs, "links": links, "cluster_basis": cluster_basis, "corner_basis": corner_basis, "corner_ids": corner_ids, "cluster_coarse": cluster_coarse, "global_coarse": global_coarse}


HIGHEST_PRECISION = lax.Precision.HIGHEST


def invert(order):
    row_index = jnp.broadcast_to(jnp.arange(order.shape[0], dtype=jnp.int32)[:, None], order.shape)
    col_index = jnp.broadcast_to(jnp.arange(order.shape[1], dtype=jnp.int32)[None, :], order.shape)
    return jnp.zeros_like(order).at[row_index, order].set(col_index)


def permuted(blocks, order):
    return jnp.take_along_axis(blocks, order[:, None, :], axis=2)


def swap(vector, tables):
    inv_up, order_down, inv_across, order_across = tables
    up_part = vector[:, :, :BLK]
    down_part = vector[:, :, BLK:2 * BLK]
    across = vector[:, :, 2 * BLK:]
    send_up = permuted(up_part, inv_up)
    send_down = permuted(down_part, order_down)
    parity = (jnp.arange(SUBS, dtype=jnp.int32) % 2) == 0
    send_across = jnp.where(parity[:, None, None], permuted(across, inv_across), permuted(across, order_across))
    layout = (CLUSTERS, N_SUB, SUB_DEV, LOADS, BLK)
    down_grid = send_down.reshape(layout)
    up_grid = send_up.reshape(layout)
    zero_rows = jnp.zeros_like(down_grid[:, :1])
    new_up = jnp.concatenate([down_grid[:, 1:], zero_rows], axis=1).reshape(SUBS, LOADS, BLK)
    new_down = jnp.concatenate([zero_rows, up_grid[:, :-1]], axis=1).reshape(SUBS, LOADS, BLK)
    paired = send_across.reshape(CLUSTERS, N_SUB, SUB_DEV // 2, 2, LOADS, BLK)
    even_part = paired[:, :, :, 0]
    odd_part = paired[:, :, :, 1]
    empty_part = jnp.zeros_like(even_part[:1])
    new_even = jnp.concatenate([odd_part[1:], empty_part], axis=0)
    new_odd = jnp.concatenate([empty_part, even_part[:-1]], axis=0)
    new_across = jnp.stack([new_even, new_odd], axis=3).reshape(SUBS, LOADS, BLK)
    return jnp.concatenate([new_up, new_down, new_across], axis=2)


def apply(vector, sign_field, operators, tables):
    spread = sign_field * (vector + swap(vector, tables))
    spread_bf = spread.astype(jnp.bfloat16)
    product = jnp.einsum("srk,skl->srl", spread_bf.astype(jnp.float32), operators.astype(jnp.float32), precision=HIGHEST_PRECISION)
    signed = sign_field * product
    result = signed + swap(signed, tables)
    curvature = jnp.sum(vector * result, axis=(0, 2))
    return result, curvature


def project(vector, cluster_basis, corner_basis, corner_ids, cluster_coarse, global_coarse):
    per_cluster = SUBS // CLUSTERS
    cluster_coef = jnp.einsum("srl,skl->srk", vector, cluster_basis, precision=HIGHEST_PRECISION)
    grouped = cluster_coef.reshape(CLUSTERS, per_cluster, LOADS, KC).transpose(0, 2, 1, 3).reshape(CLUSTERS, LOADS, CCO)
    solved = jnp.einsum("crm,cmn->crn", grouped, cluster_coarse, precision=HIGHEST_PRECISION)
    spread_back = solved.reshape(CLUSTERS, LOADS, per_cluster, KC).transpose(1, 0, 2, 3).reshape(LOADS, SUBS, KC)
    fix_cluster = jnp.einsum("rsk,skl->srl", spread_back, cluster_basis, precision=HIGHEST_PRECISION)
    flat_ids = corner_ids.reshape(-1).astype(jnp.int32)
    corner_coef = jnp.einsum("scl,srl->scr", corner_basis, vector, precision=HIGHEST_PRECISION).reshape(SUBS * CORN, LOADS)
    corner_sum = jax.ops.segment_sum(corner_coef, flat_ids, num_segments=NG)
    global_coef = jnp.dot(corner_sum.T, global_coarse, precision=HIGHEST_PRECISION)
    picked = jnp.take(global_coef, flat_ids, axis=1).reshape(LOADS, SUBS, CORN)
    fix_corner = jnp.einsum("rsc,scl->srl", picked, corner_basis, precision=HIGHEST_PRECISION)
    squares = jnp.sum(vector * vector, axis=(0, 2))
    return vector - fix_cluster - fix_corner, squares


def reference(rhs, operators, signs, links, cluster_basis, corner_basis, corner_ids, cluster_coarse, global_coarse):
    sign_field = signs.astype(jnp.float32)[:, None, :]
    tables = (invert(links[:, 0]), links[:, 1], invert(links[:, 2]), links[:, 2])
    residual = rhs
    projected, residual_norm = project(residual, cluster_basis, corner_basis, corner_ids, cluster_coarse, global_coarse)
    direction = projected
    multipliers = jnp.zeros_like(rhs)
    for iteration in range(ITERS):
        product, curvature = apply(direction, sign_field, operators, tables)
        step_size = (residual_norm / curvature)[None, :, None]
        multipliers = multipliers + step_size * direction
        residual = residual - step_size * product
        if iteration + 1 < ITERS:
            projected, norm_next = project(residual, cluster_basis, corner_basis, corner_ids, cluster_coarse, global_coarse)
            direction = projected + (norm_next / residual_norm)[None, :, None] * direction
            residual_norm = norm_next
    return multipliers, residual
```

```python
import functools

import jax
import jax.numpy as jnp
from jax import lax
from jax.experimental import pallas as pl
from jax.experimental.pallas import tpu as pltpu
from jax.sharding import PartitionSpec as P

ITERS = 2
LANES = 128
UNROLL = 8
MESH = pl.DeviceIdType.MESH
HIGHEST = lax.Precision.HIGHEST
NN = (((1,), (0,)), ((), ()))
NT = (((1,), (1,)), ((), ()))


def dot(a, b, dims=NN, precision=HIGHEST):
    return lax.dot_general(a, b, dims, precision=precision, preferred_element_type=jnp.float32)


def iota(shape, dim):
    return lax.broadcasted_iota(jnp.int32, shape, dim)


def each(count, body):
    if count <= UNROLL:
        for k in range(count):
            body(k)
    else:
        lax.fori_loop(0, count, lambda k, carry: (body(k), carry)[1], 0)


def total(ref, count, start):
    if count <= UNROLL:
        for k in range(count):
            start = start + ref[k]
        return start
    return lax.fori_loop(0, count, lambda k, acc: acc + ref[k], start)


def peer(axis, count, k):
    return lax.rem(lax.axis_index(axis) + k + 1, count)


class Spread:
    def __init__(self, axis, count, source, slots, send, recv, per_peer=False):
        self.axis, self.count, self.per_peer = axis, count, per_peer
        self.source, self.slots, self.send, self.recv = source, slots, send, recv

    def copy(self, k):
        target = peer(self.axis, self.count, k)
        source = self.source.at[target] if self.per_peer else self.source
        return pltpu.make_async_remote_copy(
            src_ref=source,
            dst_ref=self.slots.at[k],
            send_sem=self.send.at[k],
            recv_sem=self.recv.at[k],
            device_id={self.axis: target},
            device_id_type=MESH,
        )

    def start(self):
        each(self.count - 1, lambda k: self.copy(k).start())

    def wait_recv(self):
        each(self.count - 1, lambda k: self.copy(k).wait_recv())

    def wait_send(self):
        each(self.count - 1, lambda k: self.copy(k).wait_send())


def kernel(
    sizes,
    rhs_ref,
    operators_hbm,
    signs_ref,
    links_ref,
    cluster_basis_ref,
    corner_basis_ref,
    ids_ref,
    cluster_coarse_ref,
    global_coarse_ref,
    mult_ref,
    res_ref,
    ops_ref,
    ops_sem,
    basis_ref,
    weights_ref,
    global_ref,
    g_slots,
    g_send,
    g_recv,
    pick_ref,
    c_src,
    c_slots,
    c_send,
    c_recv,
    a_src,
    a_slots,
    a_send,
    a_recv,
    b_src,
    b_slots,
    b_send,
    b_recv,
    in_src,
    in_slots,
    in_send,
    in_recv,
    out_src,
    out_slots,
    out_send,
    out_recv,
    ka_src,
    ka_slots,
    ka_send,
    ka_recv,
    kb_src,
    kb_slots,
    kb_send,
    kb_recv,
):
    clusters, members = sizes
    subs, loads, dual = rhs_ref.shape
    rows = subs * loads
    kc, corn = cluster_basis_ref.shape[1], corner_basis_ref.shape[1]
    width = kc + corn
    coefs = subs * width
    order = global_coarse_ref.shape[1]
    solved = members * coefs
    my_c, my_s = lax.axis_index("cluster"), lax.axis_index("sub")

    fetch = pltpu.make_async_copy(operators_hbm, ops_ref, ops_sem)
    fetch.start()

    barrier = pltpu.get_barrier_semaphore()
    each(
        clusters - 1,
        lambda k: pl.semaphore_signal(
            barrier, inc=1, device_id={"cluster": peer("cluster", clusters, k)}, device_id_type=MESH
        ),
    )
    each(
        members - 1,
        lambda k: pl.semaphore_signal(
            barrier, inc=1, device_id={"sub": peer("sub", members, k)}, device_id_type=MESH
        ),
    )

    def field(ref):
        return jnp.concatenate([ref[s] for s in range(subs)], axis=0)

    rhs = field(rhs_ref)
    sign = jnp.concatenate(
        [
            jnp.broadcast_to(signs_ref[s : s + 1, :].astype(jnp.float32), (loads, dual))
            for s in range(subs)
        ],
        axis=0,
    )
    for s in range(subs):
        basis_ref[s * width : s * width + kc, :] = cluster_basis_ref[s]
        basis_ref[s * width + kc : (s + 1) * width, :] = corner_basis_ref[s]

    def row_of(s, b):
        return links_ref[s, b : b + 1, :]

    numbers = iota((8, LANES), 1).astype(jnp.bfloat16)

    def inverted(row):
        hot = (iota((LANES, LANES), 0) == row).astype(jnp.float32).astype(jnp.bfloat16)
        return dot(numbers, hot, NT, None)[:loads].astype(jnp.int32)

    def plain(row):
        return jnp.broadcast_to(row, (loads, LANES))

    up_order = jnp.concatenate([inverted(row_of(s, 0)) for s in range(subs)], axis=0)
    down_order = jnp.concatenate([plain(row_of(s, 1)) for s in range(subs)], axis=0)
    across_order = jnp.concatenate(
        [(plain if s % 2 else inverted)(row_of(s, 2)) for s in range(subs)], axis=0
    )

    id_row = jnp.full((1, coefs), -1, jnp.int32)
    lane = iota((1, coefs), 1)
    for s in range(subs):
        for c in range(corn):
            id_row = jnp.where(lane == s * width + kc + c, ids_ref[s, c], id_row)
    id_col = jnp.sum(
        jnp.where(iota((coefs, coefs), 0) == iota((coefs, coefs), 1), id_row, 0),
        axis=1,
        keepdims=True,
    )
    hot_rows = (id_col == iota((coefs, order), 1)).astype(jnp.float32)
    pick_ref[...] = (id_row == iota((order, coefs), 0)).astype(jnp.float32)

    where_to = iota((1, solved), 1)
    within = lax.rem(where_to, width)
    source = (
        (where_to // coefs) * (subs * kc) + (lax.rem(where_to, coefs) // width) * kc + within
    )
    source = jnp.where(within < kc, source, -1)
    place = (iota((members * subs * kc, solved), 0) == source).astype(jnp.float32)
    coarse = dot(cluster_coarse_ref[0], place)
    for s in range(subs):
        weights_ref[s * width : s * width + kc, :solved] = coarse[s * kc : (s + 1) * kc]
        weights_ref[s * width + kc : (s + 1) * width, :solved] = jnp.zeros(
            (corn, solved), jnp.float32
        )

    diagonal = iota((rows, coefs), 0) // loads == iota((rows, coefs), 1) // width

    def per_load(x):
        out = x[:loads]
        for s in range(1, subs):
            out = out + x[s * loads : (s + 1) * loads]
        return out

    def lanes_added(x):
        out = x[:, :LANES]
        for b in range(1, dual // LANES):
            out = out + x[:, b * LANES : (b + 1) * LANES]
        return out

    def tiled(x):
        return jnp.concatenate([x] * subs, axis=0)

    pl.semaphore_wait(barrier, clusters + members - 2)

    gather = Spread("sub", members, global_coarse_ref, g_slots, g_send, g_recv)
    gather.start()

    def place_global():
        depth = global_coarse_ref.shape[0]
        global_ref[pl.ds(pl.multiple_of(my_s * depth, 8), depth), :] = global_coarse_ref[...]
        gather.wait_recv()
        for k in range(members - 1):
            owner = lax.rem(my_s + 2 * members - k - 1, members)
            global_ref[pl.ds(pl.multiple_of(owner * depth, 8), depth), :] = g_slots[k]
        weights_ref[:, solved:] = dot(hot_rows, global_ref[...])

    def project(vector, n):
        raw = dot(vector, basis_ref[...], NT)
        coef = per_load(jnp.where(diagonal, raw, 0.0))
        squares = per_load(lanes_added(vector * vector))
        part = dot(coef, weights_ref[:, :solved])
        for j in range(members):
            c_src[n, j, :loads] = part[:, j * coefs : (j + 1) * coefs]
        solve = Spread(
            "sub", members, c_src.at[n], c_slots.at[n], c_send.at[n], c_recv.at[n], True
        )
        solve.start()
        if n == 0:
            place_global()
        part_global = dot(coef, weights_ref[:, solved:])
        a_src[n, :loads] = part_global
        a_src[n, loads:, :LANES] = squares
        if order > LANES:
            a_src[n, loads:, LANES:] = jnp.zeros((loads, order - LANES), jnp.float32)
        first = Spread("cluster", clusters, a_src.at[n], a_slots.at[n], a_send.at[n], a_recv.at[n])
        first.start()
        first.wait_recv()
        b_src[n] = total(a_slots.at[n], clusters - 1, a_src[n])
        second = Spread("sub", members, b_src.at[n], b_slots.at[n], b_send.at[n], b_recv.at[n])
        second.start()
        solve.wait_recv()
        own = c_src[n, my_s] + 0.0
        cluster_own = total(c_slots.at[n], members - 1, own)[:loads]
        second.wait_recv()
        both = total(b_slots.at[n], members - 1, b_src[n])
        norm = jnp.sum(both[loads : 2 * loads, :LANES], axis=1, keepdims=True)
        amount = cluster_own + dot(both[:loads], pick_ref[...])
        fix = dot(jnp.where(diagonal, tiled(amount), 0.0), basis_ref[...])
        return vector - fix, norm, (solve, first, second)

    def take(x, order_of):
        return jnp.take_along_axis(x, order_of, axis=1, mode="promise_in_bounds")

    def swap_copies(n):
        def one(src, slot, send, recv, axis, step):
            return pltpu.make_async_remote_copy(
                src_ref=src,
                dst_ref=slot,
                send_sem=send,
                recv_sem=recv,
                device_id={axis: lax.axis_index(axis) + step},
                device_id_type=MESH,
            )

        up = one(in_src.at[n, 0], in_slots.at[n, 0], in_send.at[n, 0], in_recv.at[n, 0], "sub", 1)
        down = one(
            in_src.at[n, 1], in_slots.at[n, 1], in_send.at[n, 1], in_recv.at[n, 1], "sub", -1
        )
        even = one(
            out_src.at[n, 0], out_slots.at[n, 0], out_send.at[n, 0], out_recv.at[n, 0], "cluster", 1
        )
        odd = one(
            out_src.at[n, 1], out_slots.at[n, 1], out_send.at[n, 1], out_recv.at[n, 1], "cluster", -1
        )
        return up, down, even, odd

    has_low, has_high = my_s > 0, my_s < members - 1
    has_prev, has_next = my_c > 0, my_c < clusters - 1

    def swap_start(x, n):
        across = take(x[:, 2 * LANES :], across_order)
        for p in range(2):
            for h in range(subs // 2):
                s = 2 * h + p
                out_src[n, p, h * loads : (h + 1) * loads] = across[s * loads : (s + 1) * loads]
        up, down, even, odd = swap_copies(n)
        pl.when(has_next)(even.start)
        pl.when(has_prev)(odd.start)
        in_src[n, 0] = take(x[:, :LANES], up_order)
        in_src[n, 1] = take(x[:, LANES : 2 * LANES], down_order)
        pl.when(has_high)(up.start)
        pl.when(has_low)(down.start)

    def swap_finish(n):
        up, down, even, odd = swap_copies(n)
        pl.when(has_low)(up.wait_recv)
        pl.when(has_high)(down.wait_recv)
        pl.when(has_prev)(even.wait_recv)
        pl.when(has_next)(odd.wait_recv)
        new_up = jnp.where(has_high, in_slots[n, 1], 0.0)
        new_down = jnp.where(has_low, in_slots[n, 0], 0.0)
        at_odd = jnp.where(has_prev, out_slots[n, 0], 0.0)
        at_even = jnp.where(has_next, out_slots[n, 1], 0.0)
        pieces = []
        for s in range(subs):
            h = s // 2
            pieces.append((at_odd if s % 2 else at_even)[h * loads : (h + 1) * loads])
        return jnp.concatenate([new_up, new_down, jnp.concatenate(pieces, axis=0)], axis=1)

    def swap_sent(n):
        up, down, even, odd = swap_copies(n)
        pl.when(has_high)(up.wait_send)
        pl.when(has_low)(down.wait_send)
        pl.when(has_next)(even.wait_send)
        pl.when(has_prev)(odd.wait_send)

    open_sends = []

    def apply(direction, n):
        swap_start(direction, 2 * n)
        if n == 0:
            fetch.wait()
        spread = sign * (direction + swap_finish(2 * n))
        spread_bf = spread.astype(jnp.bfloat16)
        image = jnp.concatenate(
            [
                dot(spread_bf[s * loads : (s + 1) * loads], ops_ref[s], NN, None)
                for s in range(subs)
            ],
            axis=0,
        )
        ka_src[n, :loads] = per_load(lanes_added(spread * image))
        first = Spread(
            "cluster", clusters, ka_src.at[n], ka_slots.at[n], ka_send.at[n], ka_recv.at[n]
        )
        first.start()
        signed = sign * image
        swap_start(signed, 2 * n + 1)
        first.wait_recv()
        kb_src[n] = total(ka_slots.at[n], clusters - 1, ka_src[n])
        second = Spread("sub", members, kb_src.at[n], kb_slots.at[n], kb_send.at[n], kb_recv.at[n])
        second.start()
        product = signed + swap_finish(2 * n + 1)
        second.wait_recv()
        both = total(kb_slots.at[n], members - 1, kb_src[n])
        open_sends.extend([first, second])
        return product, jnp.sum(both[:loads], axis=1, keepdims=True)

    residual = rhs
    direction, rho, open_spreads = project(residual, 0)
    open_sends.extend(open_spreads)
    multipliers = None
    for n in range(ITERS):
        product, curvature = apply(direction, n)
        step = tiled(rho / curvature)
        moved = step * direction
        multipliers = moved if multipliers is None else multipliers + moved
        residual = residual - step * product
        if n + 1 < ITERS:
            projected, rho_new, open_spreads = project(residual, n + 1)
            open_sends.extend(open_spreads)
            direction = projected + tiled(rho_new / rho) * direction
            rho = rho_new
    for s in range(subs):
        mult_ref[s] = multipliers[s * loads : (s + 1) * loads]
        res_ref[s] = residual[s * loads : (s + 1) * loads]
    gather.wait_send()
    for spread in open_sends:
        spread.wait_send()
    for n in range(2 * ITERS):
        swap_sent(n)


def local(sizes, rhs, operators, signs, links, cluster_basis, corner_basis, ids, coarse, glob):
    clusters, members = sizes
    subs, loads, dual = rhs.shape
    coefs = subs * (cluster_basis.shape[1] + corner_basis.shape[1])
    depth, order = glob.shape
    f32 = jnp.float32
    dma = pltpu.SemaphoreType.DMA

    def spread_scratch(count, peers, block, send_block=None):
        return [
            pltpu.VMEM((count,) + (send_block or block), f32),
            pltpu.VMEM((count, peers) + block, f32),
            dma((count, peers)),
            dma((count, peers)),
        ]

    vmem = pl.BlockSpec(memory_space=pltpu.VMEM)
    scratch = [
        pltpu.VMEM(operators.shape, operators.dtype),
        dma(()),
        pltpu.VMEM((coefs, dual), f32),
        pltpu.VMEM((coefs, members * coefs + order), f32),
        pltpu.VMEM((order, order), f32),
        pltpu.VMEM((members - 1, depth, order), f32),
        dma((members - 1,)),
        dma((members - 1,)),
        pltpu.VMEM((order, coefs), f32),
    ]
    scratch += spread_scratch(ITERS, members - 1, (loads, coefs), (members, loads, coefs))
    scratch += spread_scratch(ITERS, clusters - 1, (2 * loads, order))
    scratch += spread_scratch(ITERS, members - 1, (2 * loads, order))
    scratch += [
        pltpu.VMEM((2 * ITERS, 2, subs * loads, LANES), f32),
        pltpu.VMEM((2 * ITERS, 2, subs * loads, LANES), f32),
        dma((2 * ITERS, 2)),
        dma((2 * ITERS, 2)),
        pltpu.VMEM((2 * ITERS, 2, subs * loads // 2, LANES), f32),
        pltpu.VMEM((2 * ITERS, 2, subs * loads // 2, LANES), f32),
        dma((2 * ITERS, 2)),
        dma((2 * ITERS, 2)),
    ]
    scratch += spread_scratch(ITERS, clusters - 1, (loads, LANES))
    scratch += spread_scratch(ITERS, members - 1, (loads, LANES))
    return pl.pallas_call(
        functools.partial(kernel, sizes),
        out_shape=[jax.ShapeDtypeStruct(rhs.shape, f32)] * 2,
        in_specs=[
            vmem,
            pl.BlockSpec(memory_space=pl.ANY),
            vmem,
            vmem,
            vmem,
            vmem,
            pl.BlockSpec(memory_space=pltpu.SMEM),
            vmem,
            vmem,
        ],
        out_specs=[vmem, vmem],
        scratch_shapes=scratch,
        compiler_params=pltpu.CompilerParams(collective_id=0, has_side_effects=True),
    )(rhs, operators, signs, links, cluster_basis, corner_basis, ids, coarse, glob)


def solution(mesh):
    placed = (
        P(("cluster", "sub"), None, None),
        P(("cluster", "sub"), None, None),
        P(("cluster", "sub"), None),
        P(("cluster", "sub"), None, None),
        P(("cluster", "sub"), None, None),
        P(("cluster", "sub"), None, None),
        P(("cluster", "sub"), None),
        P("cluster", "sub", None),
        P("sub", None),
    )
    return jax.shard_map(
        functools.partial(local, (mesh.shape["cluster"], mesh.shape["sub"])),
        mesh=mesh,
        in_specs=placed,
        out_specs=(P(("cluster", "sub"), None, None), P(("cluster", "sub"), None, None)),
        check_vma=False,
    )
```

```python
import functools

import jax
import jax.numpy as jnp
from jax import lax
from jax.experimental import pallas as pl
from jax.experimental.pallas import tpu as pltpu
from jax.sharding import PartitionSpec as P

ITERS = 2
LANES = 128
UNROLL = 32
MESH = pl.DeviceIdType.MESH
HIGHEST = lax.Precision.HIGHEST
NN = (((1,), (0,)), ((), ()))
NT = (((1,), (1,)), ((), ()))


def dot(a, b, dims=NN, precision=HIGHEST):
    return lax.dot_general(a, b, dims, precision=precision, preferred_element_type=jnp.float32)


def iota(shape, dim):
    return lax.broadcasted_iota(jnp.int32, shape, dim)


def each(count, body):
    if count <= UNROLL:
        for k in range(count):
            body(k)
    else:
        lax.fori_loop(0, count, lambda k, carry: (body(k), carry)[1], 0)


def total(ref, count, start):
    if count <= UNROLL:
        terms = [start] + [ref[k] for k in range(count)]
        while len(terms) > 1:
            terms = [sum(terms[i : i + 2][1:], terms[i]) for i in range(0, len(terms), 2)]
        return terms[0]
    return lax.fori_loop(0, count, lambda k, acc: acc + ref[k], start)


class Spread:
    def __init__(self, sizes, axes, source, slots, send, recv):
        self.sizes, self.axes = sizes, axes
        self.source, self.slots, self.send, self.recv = source, slots, send, recv
        self.count = peers_of(sizes, axes)

    def copy(self, k):
        return pltpu.make_async_remote_copy(
            src_ref=self.source,
            dst_ref=self.slots.at[k],
            send_sem=self.send.at[k],
            recv_sem=self.recv.at[k],
            device_id=peer(self.sizes, self.axes, k),
            device_id_type=MESH,
        )

    def start(self):
        each(self.count, lambda k: self.copy(k).start())

    def wait_recv(self):
        each(self.count, lambda k: self.copy(k).wait_recv())

    def wait_send(self):
        each(self.count, lambda k: self.copy(k).wait_send())


def peers_of(sizes, axes):
    clusters, members = sizes
    return {"both": clusters * members, "cluster": clusters, "sub": members}[axes] - 1


def peer(sizes, axes, k):
    clusters, members = sizes
    if axes == "both":
        c, m = (k + 1) // members, (k + 1) % members
        return {
            "cluster": lax.rem(lax.axis_index("cluster") + c, clusters),
            "sub": lax.rem(lax.axis_index("sub") + m, members),
        }
    count = clusters if axes == "cluster" else members
    return {axes: lax.rem(lax.axis_index(axes) + k + 1, count)}


def stages(sizes):
    return ("both",) if sizes[0] * sizes[1] <= UNROLL else ("cluster", "sub")


class AllSum:
    def __init__(self, sizes, refs, n):
        self.spreads = []
        for i, axes in enumerate(stages(sizes)):
            source, slots, send, recv = refs[4 * i : 4 * i + 4]
            self.spreads.append(
                Spread(sizes, axes, source.at[n], slots.at[n], send.at[n], recv.at[n])
            )

    def start(self):
        self.spreads[0].start()

    def finish(self):
        for i, spread in enumerate(self.spreads):
            spread.wait_recv()
            out = total(spread.slots, spread.count, spread.source[...])
            if i + 1 < len(self.spreads):
                self.spreads[i + 1].source[...] = out
                self.spreads[i + 1].start()
        return out

    def wait_send(self):
        for spread in self.spreads:
            spread.wait_send()


def kernel(sizes, *refs):
    clusters, members = sizes
    hbm, out_ref, refs = refs[:9], refs[9], list(refs[10:])

    def take_refs(count):
        taken = refs[:count]
        del refs[:count]
        return taken

    local_refs = take_refs(9)
    (
        rhs_ref,
        ops_ref,
        signs_ref,
        links_ref,
        cluster_basis_ref,
        corner_basis_ref,
        ids_ref,
        cluster_coarse_ref,
        global_coarse_ref,
    ) = local_refs
    (local_sem,) = take_refs(1)
    basis_ref, weights_ref, global_ref, picked_ref, swapped_basis_ref = take_refs(5)
    g_send, g_recv = take_refs(2)
    part_refs = take_refs(4)
    piece_slots, piece_send, piece_recv = take_refs(3)
    tail_refs = take_refs(4 * len(stages(sizes)))
    curve_refs = take_refs(4 * len(stages(sizes)))
    swap_refs = take_refs(8)
    table_refs = take_refs(8)

    subs, loads, dual = rhs_ref.shape
    rows = subs * loads
    kc, corn = cluster_basis_ref.shape[1], corner_basis_ref.shape[1]
    width = kc + corn
    coefs = subs * width
    order = global_coarse_ref.shape[1]
    solved = members * coefs
    my_c, my_s = lax.axis_index("cluster"), lax.axis_index("sub")
    has_low, has_high = my_s > 0, my_s < members - 1
    has_prev, has_next = my_c > 0, my_c < clusters - 1

    barrier = pltpu.get_barrier_semaphore()

    def greet(device_id):
        pl.semaphore_signal(barrier, inc=1, device_id=device_id, device_id_type=MESH)

    greeted = 0
    for axes in ("both",) if len(stages(sizes)) == 1 else ("cluster", "sub"):
        count = peers_of(sizes, axes)
        each(count, lambda k, axes=axes: greet(peer(sizes, axes, k)))
        greeted += count
    if len(stages(sizes)) > 1:
        for there, step in ((has_next, 1), (has_prev, -1)):

            @pl.when(there)
            def _():
                for m in range(1, members):
                    greet({"cluster": my_c + step, "sub": lax.rem(my_s + m, members)})

            greeted = greeted + there.astype(jnp.int32) * (members - 1)

    loads_in = [
        pltpu.make_async_copy(hbm[i], local_refs[i], local_sem.at[i]) for i in range(len(hbm))
    ]
    for i in (6, 5, 4, 0, 7, 8, 3, 2, 1):
        loads_in[i].start()
    numbers = iota((8, LANES), 1).astype(jnp.bfloat16)

    loads_in[6].wait()
    id_row = jnp.full((1, coefs), -1, jnp.int32)
    lane = iota((1, coefs), 1)
    for s in range(subs):
        for c in range(corn):
            id_row = jnp.where(lane == s * width + kc + c, ids_ref[s, c], id_row)
    id_col = jnp.sum(
        jnp.where(iota((coefs, coefs), 0) == iota((coefs, coefs), 1), id_row, 0),
        axis=1,
        keepdims=True,
    )
    weights_ref[:, solved:] = (id_col == iota((coefs, order), 1)).astype(jnp.float32)

    loads_in[5].wait()
    loads_in[4].wait()
    for s in range(subs):
        basis_ref[s * width : s * width + kc, :] = cluster_basis_ref[s]
        basis_ref[s * width + kc : (s + 1) * width, :] = corner_basis_ref[s]

    where_to = iota((1, solved), 1)
    within = lax.rem(where_to, width)
    source = (where_to // coefs) * (subs * kc) + (lax.rem(where_to, coefs) // width) * kc + within
    source = jnp.where(within < kc, source, -1)
    place = (iota((members * subs * kc, solved), 0) == source).astype(jnp.float32)
    loads_in[0].wait()
    loads_in[7].wait()
    coarse = dot(cluster_coarse_ref[0], place)
    for s in range(subs):
        weights_ref[s * width : s * width + kc, :solved] = coarse[s * kc : (s + 1) * kc]
        weights_ref[s * width + kc : (s + 1) * width, :solved] = jnp.zeros(
            (corn, solved), jnp.float32
        )

    diagonal = iota((rows, coefs), 0) // loads == iota((rows, coefs), 1) // width
    row_sub, lane_sub = iota((rows, coefs), 0) // loads, iota((rows, coefs), 1) // width
    crossed = row_sub + 1 - 2 * lax.rem(row_sub, 2) == lane_sub

    def per_load(x):
        out = x[:loads]
        for s in range(1, subs):
            out = out + x[s * loads : (s + 1) * loads]
        return out

    def lanes_added(x):
        out = x[:, :LANES]
        for b in range(1, dual // LANES):
            out = out + x[:, b * LANES : (b + 1) * LANES]
        return out

    def tiled(x):
        return jnp.concatenate([x] * subs, axis=0)

    open_sends = []

    def piece_copy(n, side, k, step):
        target = lax.rem(my_s + k, members)
        return pltpu.make_async_remote_copy(
            src_ref=part_refs[0].at[n, target],
            dst_ref=piece_slots.at[n, side, k],
            send_sem=piece_send.at[n, side, k],
            recv_sem=piece_recv.at[n, side, k],
            device_id={"cluster": my_c + step, "sub": target},
            device_id_type=MESH,
        )

    def pieces(n, side, what):
        step = 1 - 2 * side
        for k in range(members):
            getattr(piece_copy(n, side, k, step), what)()

    def project_start(vector, n):
        raw = dot(vector, basis_ref[...], NT)
        coef = per_load(jnp.where(diagonal, raw, 0.0))
        both = dot(coef, weights_ref[...])
        tail_refs[0][n, :loads] = both[:, solved:]
        tail_refs[0][n, loads:, :LANES] = per_load(lanes_added(vector * vector))
        if order > LANES:
            tail_refs[0][n, loads:, LANES:] = jnp.zeros((loads, order - LANES), jnp.float32)
        for j in range(members):
            part_refs[0][n, j] = both[:, j * coefs : (j + 1) * coefs]
        tail = AllSum(sizes, tail_refs, n)
        tail.start()
        part = Spread(sizes, "sub", *[ref.at[n] for ref in part_refs])
        part.start()
        pl.when(has_next)(lambda: pieces(n, 0, "start"))
        pl.when(has_prev)(lambda: pieces(n, 1, "start"))
        return tail, part

    def project_finish(n, tail, part):
        part.wait_recv()
        pl.when(has_prev)(lambda: pieces(n, 0, "wait_recv"))
        pl.when(has_next)(lambda: pieces(n, 1, "wait_recv"))

        def cluster_of(member):
            out = part_refs[0][n, member]
            for k in range(members - 1):
                out = out + part_refs[1][n, k, member]
            return out

        def piece_sum(side):
            return total(piece_slots.at[n, side], members - 1, piece_slots[n, side, members - 1])

        own = cluster_of(my_s)
        high = cluster_of(jnp.minimum(my_s + 1, members - 1))
        low = cluster_of(jnp.maximum(my_s - 1, 0))
        prev, following = piece_sum(0), piece_sum(1)
        summed = tail.finish()
        open_sends.extend([tail, part])
        norm = jnp.sum(summed[loads:, :LANES], axis=1, keepdims=True)
        corners = dot(summed[:loads], picked_ref[...])

        def amount(base, i):
            return base + corners[:, i * coefs : (i + 1) * coefs]

        def block_diagonal(x, mask):
            return jnp.where(mask, tiled(x), 0.0)

        fix = dot(block_diagonal(amount(own, 0), diagonal), basis_ref[...])
        high = jnp.where(has_high, amount(high, 1), 0.0)
        low = jnp.where(has_low, amount(low, 2), 0.0)
        following = jnp.where(has_next, amount(following, 3), 0.0)
        prev = jnp.where(has_prev, amount(prev, 4), 0.0)
        odd = lax.rem(iota((loads, coefs), 1) // width, 2) == 1
        cross = jnp.where(odd, following, prev)
        fix_swapped = jnp.concatenate(
            [
                dot(block_diagonal(high, diagonal), swapped_basis_ref[0]),
                dot(block_diagonal(low, diagonal), swapped_basis_ref[1]),
                dot(block_diagonal(cross, crossed), swapped_basis_ref[2]),
            ],
            axis=1,
        )
        return fix, fix_swapped, norm

    def take(x, order_of):
        return jnp.take_along_axis(x, order_of, axis=1, mode="promise_in_bounds")

    class Swap:
        def __init__(self, refs, n):
            in_src, in_slots, in_send, in_recv, out_src, out_slots, out_send, out_recv = refs
            self.sources = [in_src.at[n, 0], in_src.at[n, 1], out_src.at[n, 0], out_src.at[n, 1]]
            self.slots = [
                in_slots.at[n, 0],
                in_slots.at[n, 1],
                out_slots.at[n, 0],
                out_slots.at[n, 1],
            ]
            self.send = [in_send.at[n, 0], in_send.at[n, 1], out_send.at[n, 0], out_send.at[n, 1]]
            self.recv = [in_recv.at[n, 0], in_recv.at[n, 1], out_recv.at[n, 0], out_recv.at[n, 1]]
            self.sends = [has_high, has_low, has_next, has_prev]
            self.takes = [has_low, has_high, has_prev, has_next]

        def copy(self, i):
            axis = "sub" if i < 2 else "cluster"
            return pltpu.make_async_remote_copy(
                src_ref=self.sources[i],
                dst_ref=self.slots[i],
                send_sem=self.send[i],
                recv_sem=self.recv[i],
                device_id={axis: lax.axis_index(axis) + (-1 if i % 2 else 1)},
                device_id_type=MESH,
            )

        def start(self, x, orders, height, extra=None):
            up_order, down_order, across_order = orders
            count = subs * height
            across = take(x[:, 2 * LANES :], across_order)
            for p in range(2):
                for h in range(subs // 2):
                    s = 2 * h + p
                    self.sources[2 + p][h * height : (h + 1) * height] = across[
                        s * height : (s + 1) * height
                    ]
            self.sources[0][:count] = take(x[:, :LANES], up_order)
            self.sources[1][:count] = take(x[:, LANES : 2 * LANES], down_order)
            if extra is not None:
                for i in range(4):
                    first = count if i < 2 else count // 2
                    self.sources[i][first : first + 8] = extra
            for i in (2, 3, 0, 1):
                pl.when(self.sends[i])(self.copy(i).start)

        def wait_recv(self):
            for i in range(4):
                pl.when(self.takes[i])(self.copy(i).wait_recv)

        def wait_send(self):
            for i in range(4):
                pl.when(self.sends[i])(self.copy(i).wait_send)

        def arrived(self, i):
            return jnp.where(self.takes[i], self.slots[i][...], 0.0)

        def field(self):
            self.wait_recv()
            at_odd, at_even = self.arrived(2), self.arrived(3)
            across = [
                (at_odd if s % 2 else at_even)[s // 2 * loads : (s // 2 + 1) * loads]
                for s in range(subs)
            ]
            return jnp.concatenate(
                [self.arrived(1), self.arrived(0), jnp.concatenate(across, axis=0)], axis=1
            )

    depth = global_coarse_ref.shape[0]
    own_rows = pl.ds(pl.multiple_of(my_s * depth, 8), depth)

    def gather_copy(k):
        return pltpu.make_async_remote_copy(
            src_ref=global_coarse_ref,
            dst_ref=global_ref.at[own_rows],
            send_sem=g_send.at[k],
            recv_sem=g_recv.at[k],
            device_id=peer(sizes, "sub", k),
            device_id_type=MESH,
        )

    def begin():
        loads_in[8].wait()
        global_ref[own_rows, :] = global_coarse_ref[...]
        each(members - 1, lambda k: gather_copy(k).start())
        loads_in[3].wait()

        def plain(row):
            return row

        def inverted(row):
            hot = (iota((LANES, LANES), 0) == row).astype(jnp.float32).astype(jnp.bfloat16)
            return dot(numbers, hot, NT, None)[:1].astype(jnp.int32)

        index = [
            [inverted(links_ref[0, s : s + 1, :]) for s in range(subs)],
            [plain(links_ref[1, s : s + 1, :]) for s in range(subs)],
            [(plain if s % 2 else inverted)(links_ref[2, s : s + 1, :]) for s in range(subs)],
        ]

        def orders_of(height):
            return [
                jnp.concatenate(
                    [jnp.broadcast_to(row, (height, LANES)) for row in block], axis=0
                )
                for block in index
            ]

        orders = orders_of(loads)
        rhs_swap = Swap(swap_refs, ITERS)
        rhs_swap.start(rhs, orders, loads)
        tables = Swap(table_refs, 0)
        ids_sent = jnp.broadcast_to(id_row.astype(jnp.float32), (8, coefs))
        tables.start(basis_ref[...], orders_of(width), width, ids_sent)

        loads_in[2].wait()
        sign = jnp.concatenate(
            [
                jnp.broadcast_to(signs_ref[s : s + 1, :].astype(jnp.float32), (loads, dual))
                for s in range(subs)
            ],
            axis=0,
        )
        each(members - 1, lambda k: gather_copy(k).wait_recv())
        tables.wait_recv()
        swapped_basis_ref[0] = tables.arrived(1)[:coefs]
        swapped_basis_ref[1] = tables.arrived(0)[:coefs]
        from_prev, from_next = tables.arrived(2), tables.arrived(3)
        for s in range(subs):
            swapped_basis_ref[2, s * width : (s + 1) * width] = (
                from_next if s % 2 else from_prev
            )[s // 2 * width : (s // 2 + 1) * width]
        id_rows = [id_row.astype(jnp.float32)]
        for i in (1, 0, 3, 2):
            first = coefs if i < 2 else coefs // 2
            id_rows.append(tables.slots[i][first : first + 1])
        whose = iota((order, coefs), 0).astype(jnp.float32)
        picks = jnp.concatenate([(row == whose).astype(jnp.float32) for row in id_rows], axis=1)
        for r in range(0, order, 2 * LANES):
            chunk = slice(r, min(r + 2 * LANES, order))
            picked_ref[chunk] = dot(global_ref[chunk], picks)
        loads_in[1].wait()
        open_sends.extend([rhs_swap, tables])
        return sign, orders, rhs_swap.field()

    rhs = jnp.concatenate([rhs_ref[s] for s in range(subs)], axis=0)
    pl.semaphore_wait(barrier, greeted)
    started = project_start(rhs, 0)
    sign, orders, residual_swapped = begin()
    fix, fix_swapped, rho = project_finish(0, *started)
    residual = rhs
    direction, direction_swapped = residual - fix, residual_swapped - fix_swapped
    row_odd = lax.rem(iota((rows, LANES), 0) // loads, 2) == 1
    there = jnp.concatenate(
        [
            jnp.full((rows, LANES), has_high.astype(jnp.float32)),
            jnp.full((rows, LANES), has_low.astype(jnp.float32)),
            jnp.where(row_odd, has_prev.astype(jnp.float32), has_next.astype(jnp.float32)),
        ],
        axis=1,
    )
    multipliers = None
    for n in range(ITERS):
        spread = sign * (direction + direction_swapped)
        spread_bf = spread.astype(jnp.bfloat16)
        image = jnp.concatenate(
            [
                dot(spread_bf[s * loads : (s + 1) * loads], ops_ref[s], NN, None)
                for s in range(subs)
            ],
            axis=0,
        )
        curve_refs[0][n] = per_load(lanes_added(spread * image))
        curve = AllSum(sizes, curve_refs, n)
        curve.start()
        signed = sign * image
        swap = Swap(swap_refs, n)
        swap.start(signed, orders, loads)
        signed_swapped = swap.field()
        product = signed + signed_swapped
        product_swapped = signed_swapped + there * signed
        curvature = jnp.sum(curve.finish(), axis=1, keepdims=True)
        open_sends.extend([curve, swap])
        step = tiled(rho / curvature)
        residual = residual - step * product
        if n + 1 < ITERS:
            started = project_start(residual, n + 1)
        moved = step * direction
        multipliers = moved if multipliers is None else multipliers + moved
        if n + 1 < ITERS:
            residual_swapped = residual_swapped - step * product_swapped
            fix, fix_swapped, rho_new = project_finish(n + 1, *started)
            ratio = tiled(rho_new / rho)
            direction = residual - fix + ratio * direction
            direction_swapped = residual_swapped - fix_swapped + ratio * direction_swapped
            rho = rho_new
    for s in range(subs):
        out_ref[0, s] = multipliers[s * loads : (s + 1) * loads]
        out_ref[1, s] = residual[s * loads : (s + 1) * loads]
    for spread in open_sends:
        spread.wait_send()
    each(members - 1, lambda k: gather_copy(k).wait_send())
    for n in range(ITERS):
        pl.when(has_next)(lambda n=n: pieces(n, 0, "wait_send"))
        pl.when(has_prev)(lambda n=n: pieces(n, 1, "wait_send"))


def split(both_ref, mult_ref, res_ref):
    mult_ref[...] = both_ref[0]
    res_ref[...] = both_ref[1]


def local(sizes, *args):
    args = list(args)
    args[3] = jnp.transpose(args[3], (1, 0, 2))
    rhs, operators, signs, links, cluster_basis, corner_basis, ids, coarse, glob = args
    clusters, members = sizes
    subs, loads, dual = rhs.shape
    coefs = subs * (cluster_basis.shape[1] + corner_basis.shape[1])
    depth, order = glob.shape
    f32 = jnp.float32
    dma = pltpu.SemaphoreType.DMA

    def exchange(lead, block, receive):
        return [
            pltpu.VMEM(lead[:1] + block, f32),
            pltpu.VMEM(lead + receive, f32),
            dma(lead),
            dma(lead),
        ]

    def swap_scratch(count, height, extra):
        scratch = []
        for rows in (subs * height + extra, subs * height // 2 + extra):
            scratch += [
                pltpu.VMEM((count, 2, rows, LANES), f32),
                pltpu.VMEM((count, 2, rows, LANES), f32),
                dma((count, 2)),
                dma((count, 2)),
            ]
        return scratch

    def sum_scratch(block):
        scratch = []
        for axes in stages(sizes):
            scratch += exchange((ITERS, peers_of(sizes, axes)), block, block)
        return scratch

    vmem = pl.BlockSpec(memory_space=pltpu.VMEM)
    scratch = [pltpu.VMEM(a.shape, a.dtype) for a in args]
    scratch[6] = pltpu.SMEM(ids.shape, ids.dtype)
    scratch += [
        dma((len(args),)),
        pltpu.VMEM((coefs, dual), f32),
        pltpu.VMEM((coefs, members * coefs + order), f32),
        pltpu.VMEM((order, order), f32),
        pltpu.VMEM((order, 5 * coefs), f32),
        pltpu.VMEM((3, coefs, LANES), f32),
        dma((members - 1,)),
        dma((members - 1,)),
    ]
    part = (members, loads, coefs)
    scratch += exchange((ITERS, members - 1), part, part)
    scratch += [
        pltpu.VMEM((ITERS, 2, members, loads, coefs), f32),
        dma((ITERS, 2, members)),
        dma((ITERS, 2, members)),
    ]
    scratch += sum_scratch((2 * loads, order)) + sum_scratch((loads, LANES))
    scratch += swap_scratch(ITERS + 1, loads, 0)
    scratch += swap_scratch(1, coefs // subs, 8)
    both = pl.pallas_call(
        functools.partial(kernel, sizes),
        out_shape=jax.ShapeDtypeStruct((2,) + rhs.shape, f32),
        in_specs=[pl.BlockSpec(memory_space=pl.ANY)] * len(args),
        out_specs=vmem,
        scratch_shapes=scratch,
        compiler_params=pltpu.CompilerParams(collective_id=0, has_side_effects=True),
    )(*args)
    return pl.pallas_call(
        split,
        out_shape=[jax.ShapeDtypeStruct(rhs.shape, f32)] * 2,
        in_specs=[vmem],
        out_specs=[vmem, vmem],
    )(both)


def solution(mesh):
    placed = (
        P(("cluster", "sub"), None, None),
        P(("cluster", "sub"), None, None),
        P(("cluster", "sub"), None),
        P(("cluster", "sub"), None, None),
        P(("cluster", "sub"), None, None),
        P(("cluster", "sub"), None, None),
        P(("cluster", "sub"), None),
        P("cluster", "sub", None),
        P("sub", None),
    )
    return jax.shard_map(
        functools.partial(local, (mesh.shape["cluster"], mesh.shape["sub"])),
        mesh=mesh,
        in_specs=placed,
        out_specs=(P(("cluster", "sub"), None, None), P(("cluster", "sub"), None, None)),
        check_vma=False,
    )
```

```python
import functools

import jax
import jax.numpy as jnp
from jax import lax
from jax.experimental import pallas as pl
from jax.experimental.pallas import tpu as pltpu
from jax.sharding import PartitionSpec as P

ITERS = 2
LANES = 128
UNROLL = 32
MESH = pl.DeviceIdType.MESH
HIGHEST = lax.Precision.HIGHEST
NN = (((1,), (0,)), ((), ()))
NT = (((1,), (1,)), ((), ()))


def dot(a, b, dims=NN, precision=HIGHEST):
    return lax.dot_general(a, b, dims, precision=precision, preferred_element_type=jnp.float32)


def iota(shape, dim):
    return lax.broadcasted_iota(jnp.int32, shape, dim)


def each(count, body):
    if count <= UNROLL:
        for k in range(count):
            body(k)
    else:
        lax.fori_loop(0, count, lambda k, carry: (body(k), carry)[1], 0)


def total(ref, count, start):
    if count <= UNROLL:
        terms = [start] + [ref[k] for k in range(count)]
        while len(terms) > 1:
            terms = [sum(terms[i : i + 2][1:], terms[i]) for i in range(0, len(terms), 2)]
        return terms[0]
    return lax.fori_loop(0, count, lambda k, acc: acc + ref[k], start)


class Spread:
    def __init__(self, sizes, axes, source, slots, send, recv):
        self.sizes, self.axes = sizes, axes
        self.source, self.slots, self.send, self.recv = source, slots, send, recv
        self.count = peers_of(sizes, axes)

    def copy(self, k):
        return pltpu.make_async_remote_copy(
            src_ref=self.source,
            dst_ref=self.slots.at[k],
            send_sem=self.send.at[k],
            recv_sem=self.recv.at[k],
            device_id=peer(self.sizes, self.axes, k),
            device_id_type=MESH,
        )

    def start(self):
        each(self.count, lambda k: self.copy(k).start())

    def wait_recv(self):
        each(self.count, lambda k: self.copy(k).wait_recv())

    def wait_send(self):
        each(self.count, lambda k: self.copy(k).wait_send())


def peers_of(sizes, axes):
    clusters, members = sizes
    return {"both": clusters * members, "cluster": clusters, "sub": members}[axes] - 1


def peer(sizes, axes, k):
    clusters, members = sizes
    if axes == "both":
        c, m = (k + 1) // members, (k + 1) % members
        return {
            "cluster": lax.rem(lax.axis_index("cluster") + c, clusters),
            "sub": lax.rem(lax.axis_index("sub") + m, members),
        }
    count = clusters if axes == "cluster" else members
    return {axes: lax.rem(lax.axis_index(axes) + k + 1, count)}


def stages(sizes):
    return ("both",) if sizes[0] * sizes[1] <= UNROLL else ("cluster", "sub")


class AllSum:
    def __init__(self, sizes, refs, n):
        self.spreads = []
        for i, axes in enumerate(stages(sizes)):
            source, slots, send, recv = refs[4 * i : 4 * i + 4]
            self.spreads.append(
                Spread(sizes, axes, source.at[n], slots.at[n], send.at[n], recv.at[n])
            )

    def start(self):
        self.spreads[0].start()

    def finish(self):
        for i, spread in enumerate(self.spreads):
            spread.wait_recv()
            out = total(spread.slots, spread.count, spread.source[...])
            if i + 1 < len(self.spreads):
                self.spreads[i + 1].source[...] = out
                self.spreads[i + 1].start()
        return out

    def wait_send(self):
        for spread in self.spreads:
            spread.wait_send()


def kernel(sizes, *refs):
    clusters, members = sizes
    hbm, out_ref, refs = refs[:9], refs[9], list(refs[10:])

    def take_refs(count):
        taken = refs[:count]
        del refs[:count]
        return taken

    local_refs = take_refs(9)
    (
        rhs_ref,
        ops_ref,
        signs_ref,
        links_ref,
        cluster_basis_ref,
        corner_basis_ref,
        ids_ref,
        cluster_coarse_ref,
        global_coarse_ref,
    ) = local_refs
    (local_sem,) = take_refs(1)
    basis_ref, weights_ref, global_ref, picked_ref, swapped_basis_ref = take_refs(5)
    g_send, g_recv = take_refs(2)
    part_refs = take_refs(4)
    piece_slots, piece_send, piece_recv = take_refs(3)
    tail_refs = take_refs(4 * len(stages(sizes)))
    curve_refs = take_refs(4 * len(stages(sizes)))
    swap_refs = take_refs(8)
    table_refs = take_refs(8)

    subs, loads, dual = rhs_ref.shape
    rows = subs * loads
    kc, corn = cluster_basis_ref.shape[1], corner_basis_ref.shape[1]
    width = kc + corn
    coefs = subs * width
    order = global_coarse_ref.shape[1]
    solved = members * coefs
    my_c, my_s = lax.axis_index("cluster"), lax.axis_index("sub")
    has_low, has_high = my_s > 0, my_s < members - 1
    has_prev, has_next = my_c > 0, my_c < clusters - 1

    barrier = pltpu.get_barrier_semaphore()

    def greet(device_id):
        pl.semaphore_signal(barrier, inc=1, device_id=device_id, device_id_type=MESH)

    greeted = 0
    for axes in ("both",) if len(stages(sizes)) == 1 else ("cluster", "sub"):
        count = peers_of(sizes, axes)
        each(count, lambda k, axes=axes: greet(peer(sizes, axes, k)))
        greeted += count
    if len(stages(sizes)) > 1:
        for there, step in ((has_next, 1), (has_prev, -1)):

            @pl.when(there)
            def _():
                for m in range(1, members):
                    greet({"cluster": my_c + step, "sub": lax.rem(my_s + m, members)})

            greeted = greeted + there.astype(jnp.int32) * (members - 1)

    loads_in = [
        pltpu.make_async_copy(hbm[i], local_refs[i], local_sem.at[i]) for i in range(len(hbm))
    ]
    for i in (6, 5, 4, 0, 7, 8, 3, 2, 1):
        loads_in[i].start()
    numbers = iota((8, LANES), 1).astype(jnp.bfloat16)

    loads_in[6].wait()
    id_row = jnp.full((1, coefs), -1, jnp.int32)
    lane = iota((1, coefs), 1)
    for s in range(subs):
        for c in range(corn):
            id_row = jnp.where(lane == s * width + kc + c, ids_ref[s, c], id_row)
    id_col = jnp.sum(
        jnp.where(iota((coefs, coefs), 0) == iota((coefs, coefs), 1), id_row, 0),
        axis=1,
        keepdims=True,
    )
    weights_ref[:, solved:] = (id_col == iota((coefs, order), 1)).astype(jnp.float32)

    loads_in[5].wait()
    loads_in[4].wait()
    for s in range(subs):
        basis_ref[s * width : s * width + kc, :] = cluster_basis_ref[s]
        basis_ref[s * width + kc : (s + 1) * width, :] = corner_basis_ref[s]

    where_to = iota((1, solved), 1)
    within = lax.rem(where_to, width)
    source = (where_to // coefs) * (subs * kc) + (lax.rem(where_to, coefs) // width) * kc + within
    source = jnp.where(within < kc, source, -1)
    place = (iota((members * subs * kc, solved), 0) == source).astype(jnp.float32)
    loads_in[0].wait()
    loads_in[7].wait()
    coarse = dot(cluster_coarse_ref[0], place)
    for s in range(subs):
        weights_ref[s * width : s * width + kc, :solved] = coarse[s * kc : (s + 1) * kc]
        weights_ref[s * width + kc : (s + 1) * width, :solved] = jnp.zeros(
            (corn, solved), jnp.float32
        )

    diagonal = iota((rows, coefs), 0) // loads == iota((rows, coefs), 1) // width
    row_sub, lane_sub = iota((rows, coefs), 0) // loads, iota((rows, coefs), 1) // width
    crossed = row_sub + 1 - 2 * lax.rem(row_sub, 2) == lane_sub

    def per_load(x):
        out = x[:loads]
        for s in range(1, subs):
            out = out + x[s * loads : (s + 1) * loads]
        return out

    def lanes_added(x):
        out = x[:, :LANES]
        for b in range(1, dual // LANES):
            out = out + x[:, b * LANES : (b + 1) * LANES]
        return out

    def tiled(x):
        return jnp.concatenate([x] * subs, axis=0)

    lane_is_load = iota((loads, LANES), 0) == iota((loads, LANES), 1)

    def as_row(x):
        sums = jnp.sum(x, axis=1, keepdims=True)
        return jnp.sum(jnp.where(lane_is_load, sums, 0.0), axis=0, keepdims=True)

    def as_column(x):
        return jnp.sum(jnp.where(lane_is_load, x, 0.0), axis=1, keepdims=True)

    open_sends = []

    def piece_copy(n, side, k, step):
        target = lax.rem(my_s + k, members)
        return pltpu.make_async_remote_copy(
            src_ref=part_refs[0].at[n, target],
            dst_ref=piece_slots.at[n, side, k],
            send_sem=piece_send.at[n, side, k],
            recv_sem=piece_recv.at[n, side, k],
            device_id={"cluster": my_c + step, "sub": target},
            device_id_type=MESH,
        )

    def pieces(n, side, what):
        step = 1 - 2 * side
        for k in range(members):
            getattr(piece_copy(n, side, k, step), what)()

    def project_start(vector, n):
        raw = dot(vector, basis_ref[...], NT)
        coef = per_load(jnp.where(diagonal, raw, 0.0))
        both = dot(coef, weights_ref[...])
        tail_refs[0][n, :loads] = both[:, solved:]
        tail_refs[0][n, loads:, :LANES] = as_row(per_load(lanes_added(vector * vector)))
        if order > LANES:
            tail_refs[0][n, loads:, LANES:] = jnp.zeros((1, order - LANES), jnp.float32)
        for j in range(members):
            part_refs[0][n, j] = both[:, j * coefs : (j + 1) * coefs]
        tail = AllSum(sizes, tail_refs, n)
        tail.start()
        part = Spread(sizes, "sub", *[ref.at[n] for ref in part_refs])
        part.start()
        pl.when(has_next)(lambda: pieces(n, 0, "start"))
        pl.when(has_prev)(lambda: pieces(n, 1, "start"))
        return tail, part

    def project_finish(n, tail, part):
        part.wait_recv()
        pl.when(has_prev)(lambda: pieces(n, 0, "wait_recv"))
        pl.when(has_next)(lambda: pieces(n, 1, "wait_recv"))

        def cluster_of(member):
            out = part_refs[0][n, member]
            for k in range(members - 1):
                out = out + part_refs[1][n, k, member]
            return out

        def piece_sum(side):
            return total(piece_slots.at[n, side], members - 1, piece_slots[n, side, members - 1])

        own = cluster_of(my_s)
        high = cluster_of(jnp.minimum(my_s + 1, members - 1))
        low = cluster_of(jnp.maximum(my_s - 1, 0))
        prev, following = piece_sum(0), piece_sum(1)
        summed = tail.finish()
        open_sends.extend([tail, part])
        norm = as_column(summed[loads:, :LANES])
        corners = dot(summed[:loads], picked_ref[...])

        def amount(base, i):
            return base + corners[:, i * coefs : (i + 1) * coefs]

        def block_diagonal(x, mask):
            return jnp.where(mask, tiled(x), 0.0)

        fix = dot(block_diagonal(amount(own, 0), diagonal), basis_ref[...])
        high = jnp.where(has_high, amount(high, 1), 0.0)
        low = jnp.where(has_low, amount(low, 2), 0.0)
        following = jnp.where(has_next, amount(following, 3), 0.0)
        prev = jnp.where(has_prev, amount(prev, 4), 0.0)
        odd = lax.rem(iota((loads, coefs), 1) // width, 2) == 1
        cross = jnp.where(odd, following, prev)
        fix_swapped = jnp.concatenate(
            [
                dot(block_diagonal(high, diagonal), swapped_basis_ref[0]),
                dot(block_diagonal(low, diagonal), swapped_basis_ref[1]),
                dot(block_diagonal(cross, crossed), swapped_basis_ref[2]),
            ],
            axis=1,
        )
        return fix, fix_swapped, norm

    def take(x, order_of):
        return jnp.take_along_axis(x, order_of, axis=1, mode="promise_in_bounds")

    class Swap:
        def __init__(self, refs, n):
            in_src, in_slots, in_send, in_recv, out_src, out_slots, out_send, out_recv = refs
            self.sources = [in_src.at[n, 0], in_src.at[n, 1], out_src.at[n, 0], out_src.at[n, 1]]
            self.slots = [
                in_slots.at[n, 0],
                in_slots.at[n, 1],
                out_slots.at[n, 0],
                out_slots.at[n, 1],
            ]
            self.send = [in_send.at[n, 0], in_send.at[n, 1], out_send.at[n, 0], out_send.at[n, 1]]
            self.recv = [in_recv.at[n, 0], in_recv.at[n, 1], out_recv.at[n, 0], out_recv.at[n, 1]]
            self.sends = [has_high, has_low, has_next, has_prev]
            self.takes = [has_low, has_high, has_prev, has_next]

        def copy(self, i):
            axis = "sub" if i < 2 else "cluster"
            return pltpu.make_async_remote_copy(
                src_ref=self.sources[i],
                dst_ref=self.slots[i],
                send_sem=self.send[i],
                recv_sem=self.recv[i],
                device_id={axis: lax.axis_index(axis) + (-1 if i % 2 else 1)},
                device_id_type=MESH,
            )

        def start(self, x, orders, height, extra=None):
            up_order, down_order, across_order = orders
            count = subs * height
            across = take(x[:, 2 * LANES :], across_order)
            for p in range(2):
                for h in range(subs // 2):
                    s = 2 * h + p
                    self.sources[2 + p][h * height : (h + 1) * height] = across[
                        s * height : (s + 1) * height
                    ]
            self.sources[0][:count] = take(x[:, :LANES], up_order)
            self.sources[1][:count] = take(x[:, LANES : 2 * LANES], down_order)
            if extra is not None:
                for i in range(4):
                    first = count if i < 2 else count // 2
                    self.sources[i][first : first + 8] = extra
            for i in (2, 3, 0, 1):
                pl.when(self.sends[i])(self.copy(i).start)

        def wait_recv(self):
            for i in range(4):
                pl.when(self.takes[i])(self.copy(i).wait_recv)

        def wait_send(self):
            for i in range(4):
                pl.when(self.sends[i])(self.copy(i).wait_send)

        def arrived(self, i):
            return jnp.where(self.takes[i], self.slots[i][...], 0.0)

        def field(self):
            self.wait_recv()
            at_odd, at_even = self.arrived(2), self.arrived(3)
            across = [
                (at_odd if s % 2 else at_even)[s // 2 * loads : (s // 2 + 1) * loads]
                for s in range(subs)
            ]
            return jnp.concatenate(
                [self.arrived(1), self.arrived(0), jnp.concatenate(across, axis=0)], axis=1
            )

    depth = global_coarse_ref.shape[0]
    own_rows = pl.ds(pl.multiple_of(my_s * depth, 8), depth)

    def gather_copy(k):
        return pltpu.make_async_remote_copy(
            src_ref=global_coarse_ref,
            dst_ref=global_ref.at[own_rows],
            send_sem=g_send.at[k],
            recv_sem=g_recv.at[k],
            device_id=peer(sizes, "sub", k),
            device_id_type=MESH,
        )

    def begin():
        loads_in[8].wait()
        global_ref[own_rows, :] = global_coarse_ref[...]
        each(members - 1, lambda k: gather_copy(k).start())
        loads_in[3].wait()

        def plain(row):
            return row

        def inverted(row):
            hot = (iota((LANES, LANES), 0) == row).astype(jnp.float32).astype(jnp.bfloat16)
            return dot(numbers, hot, NT, None)[:1].astype(jnp.int32)

        index = [
            [inverted(links_ref[0, s : s + 1, :]) for s in range(subs)],
            [plain(links_ref[1, s : s + 1, :]) for s in range(subs)],
            [(plain if s % 2 else inverted)(links_ref[2, s : s + 1, :]) for s in range(subs)],
        ]

        def orders_of(height):
            return [
                jnp.concatenate(
                    [jnp.broadcast_to(row, (height, LANES)) for row in block], axis=0
                )
                for block in index
            ]

        orders = orders_of(loads)
        rhs_swap = Swap(swap_refs, ITERS)
        rhs_swap.start(rhs, orders, loads)
        tables = Swap(table_refs, 0)
        ids_sent = jnp.broadcast_to(id_row.astype(jnp.float32), (8, coefs))
        tables.start(basis_ref[...], orders_of(width), width, ids_sent)

        loads_in[2].wait()
        sign = jnp.concatenate(
            [
                jnp.broadcast_to(signs_ref[s : s + 1, :].astype(jnp.float32), (loads, dual))
                for s in range(subs)
            ],
            axis=0,
        )
        each(members - 1, lambda k: gather_copy(k).wait_recv())
        tables.wait_recv()
        swapped_basis_ref[0] = tables.arrived(1)[:coefs]
        swapped_basis_ref[1] = tables.arrived(0)[:coefs]
        from_prev, from_next = tables.arrived(2), tables.arrived(3)
        for s in range(subs):
            swapped_basis_ref[2, s * width : (s + 1) * width] = (
                from_next if s % 2 else from_prev
            )[s // 2 * width : (s // 2 + 1) * width]
        id_rows = [id_row.astype(jnp.float32)]
        for i in (1, 0, 3, 2):
            first = coefs if i < 2 else coefs // 2
            id_rows.append(tables.slots[i][first : first + 1])
        whose = iota((order, coefs), 0).astype(jnp.float32)
        picks = jnp.concatenate([(row == whose).astype(jnp.float32) for row in id_rows], axis=1)
        for r in range(0, order, 2 * LANES):
            chunk = slice(r, min(r + 2 * LANES, order))
            picked_ref[chunk] = dot(global_ref[chunk], picks)
        loads_in[1].wait()
        open_sends.extend([rhs_swap, tables])
        return sign, orders, rhs_swap.field()

    rhs = jnp.concatenate([rhs_ref[s] for s in range(subs)], axis=0)
    pl.semaphore_wait(barrier, greeted)
    started = project_start(rhs, 0)
    sign, orders, residual_swapped = begin()
    fix, fix_swapped, rho = project_finish(0, *started)
    residual = rhs
    direction, direction_swapped = residual - fix, residual_swapped - fix_swapped
    row_odd = lax.rem(iota((rows, LANES), 0) // loads, 2) == 1
    there = jnp.concatenate(
        [
            jnp.full((rows, LANES), has_high.astype(jnp.float32)),
            jnp.full((rows, LANES), has_low.astype(jnp.float32)),
            jnp.where(row_odd, has_prev.astype(jnp.float32), has_next.astype(jnp.float32)),
        ],
        axis=1,
    )
    multipliers = None
    for n in range(ITERS):
        spread = sign * (direction + direction_swapped)
        spread_bf = spread.astype(jnp.bfloat16)
        image = jnp.concatenate(
            [
                dot(spread_bf[s * loads : (s + 1) * loads], ops_ref[s], NN, None)
                for s in range(subs)
            ],
            axis=0,
        )
        curve_refs[0][n] = as_row(per_load(lanes_added(spread * image)))
        curve = AllSum(sizes, curve_refs, n)
        curve.start()
        signed = sign * image
        swap = Swap(swap_refs, n)
        swap.start(signed, orders, loads)
        signed_swapped = swap.field()
        product = signed + signed_swapped
        product_swapped = signed_swapped + there * signed
        curvature = as_column(curve.finish())
        open_sends.extend([curve, swap])
        step = tiled(rho / curvature)
        residual = residual - step * product
        if n + 1 < ITERS:
            started = project_start(residual, n + 1)
        moved = step * direction
        multipliers = moved if multipliers is None else multipliers + moved
        if n + 1 < ITERS:
            residual_swapped = residual_swapped - step * product_swapped
            fix, fix_swapped, rho_new = project_finish(n + 1, *started)
            ratio = tiled(rho_new / rho)
            direction = residual - fix + ratio * direction
            direction_swapped = residual_swapped - fix_swapped + ratio * direction_swapped
            rho = rho_new
    for s in range(subs):
        out_ref[0, s] = multipliers[s * loads : (s + 1) * loads]
        out_ref[1, s] = residual[s * loads : (s + 1) * loads]
    for spread in open_sends:
        spread.wait_send()
    each(members - 1, lambda k: gather_copy(k).wait_send())
    for n in range(ITERS):
        pl.when(has_next)(lambda n=n: pieces(n, 0, "wait_send"))
        pl.when(has_prev)(lambda n=n: pieces(n, 1, "wait_send"))


def split(both_ref, mult_ref, res_ref):
    mult_ref[...] = both_ref[0]
    res_ref[...] = both_ref[1]


def local(sizes, *args):
    args = list(args)
    args[3] = jnp.transpose(args[3], (1, 0, 2))
    rhs, operators, signs, links, cluster_basis, corner_basis, ids, coarse, glob = args
    clusters, members = sizes
    subs, loads, dual = rhs.shape
    coefs = subs * (cluster_basis.shape[1] + corner_basis.shape[1])
    depth, order = glob.shape
    f32 = jnp.float32
    dma = pltpu.SemaphoreType.DMA

    def exchange(lead, block, receive):
        return [
            pltpu.VMEM(lead[:1] + block, f32),
            pltpu.VMEM(lead + receive, f32),
            dma(lead),
            dma(lead),
        ]

    def swap_scratch(count, height, extra):
        scratch = []
        for rows in (subs * height + extra, subs * height // 2 + extra):
            scratch += [
                pltpu.VMEM((count, 2, rows, LANES), f32),
                pltpu.VMEM((count, 2, rows, LANES), f32),
                dma((count, 2)),
                dma((count, 2)),
            ]
        return scratch

    def sum_scratch(block):
        scratch = []
        for axes in stages(sizes):
            scratch += exchange((ITERS, peers_of(sizes, axes)), block, block)
        return scratch

    vmem = pl.BlockSpec(memory_space=pltpu.VMEM)
    scratch = [pltpu.VMEM(a.shape, a.dtype) for a in args]
    scratch[6] = pltpu.SMEM(ids.shape, ids.dtype)
    scratch += [
        dma((len(args),)),
        pltpu.VMEM((coefs, dual), f32),
        pltpu.VMEM((coefs, members * coefs + order), f32),
        pltpu.VMEM((order, order), f32),
        pltpu.VMEM((order, 5 * coefs), f32),
        pltpu.VMEM((3, coefs, LANES), f32),
        dma((members - 1,)),
        dma((members - 1,)),
    ]
    part = (members, loads, coefs)
    scratch += exchange((ITERS, members - 1), part, part)
    scratch += [
        pltpu.VMEM((ITERS, 2, members, loads, coefs), f32),
        dma((ITERS, 2, members)),
        dma((ITERS, 2, members)),
    ]
    scratch += sum_scratch((loads + 1, order)) + sum_scratch((1, LANES))
    scratch += swap_scratch(ITERS + 1, loads, 0)
    scratch += swap_scratch(1, coefs // subs, 8)
    both = pl.pallas_call(
        functools.partial(kernel, sizes),
        out_shape=jax.ShapeDtypeStruct((2,) + rhs.shape, f32),
        in_specs=[pl.BlockSpec(memory_space=pl.ANY)] * len(args),
        out_specs=vmem,
        scratch_shapes=scratch,
        compiler_params=pltpu.CompilerParams(collective_id=0, has_side_effects=True),
    )(*args)
    return pl.pallas_call(
        split,
        out_shape=[jax.ShapeDtypeStruct(rhs.shape, f32)] * 2,
        in_specs=[vmem],
        out_specs=[vmem, vmem],
    )(both)


def solution(mesh):
    placed = (
        P(("cluster", "sub"), None, None),
        P(("cluster", "sub"), None, None),
        P(("cluster", "sub"), None),
        P(("cluster", "sub"), None, None),
        P(("cluster", "sub"), None, None),
        P(("cluster", "sub"), None, None),
        P(("cluster", "sub"), None),
        P("cluster", "sub", None),
        P("sub", None),
    )
    return jax.shard_map(
        functools.partial(local, (mesh.shape["cluster"], mesh.shape["sub"])),
        mesh=mesh,
        in_specs=placed,
        out_specs=(P(("cluster", "sub"), None, None), P(("cluster", "sub"), None, None)),
        check_vma=False,
    )
```

```python
import functools

import jax
import jax.numpy as jnp
from jax import lax
from jax.experimental import pallas as pl
from jax.experimental.pallas import tpu as pltpu
from jax.sharding import PartitionSpec as P

ITERS = 2
LANES = 128
UNROLL = 32
MESH = pl.DeviceIdType.MESH
HIGHEST = lax.Precision.HIGHEST
NN = (((1,), (0,)), ((), ()))
NT = (((1,), (1,)), ((), ()))


def dot(a, b, dims=NN, precision=HIGHEST):
    return lax.dot_general(a, b, dims, precision=precision, preferred_element_type=jnp.float32)


def dot3(a, b, dims=NN):
    bf16, f32 = jnp.bfloat16, jnp.float32
    rows = a.shape[0]
    a_high, b_high = a.astype(bf16).astype(f32), b.astype(bf16)
    b_low = (b - b_high.astype(f32)).astype(bf16)
    halves = jnp.concatenate([a_high, a - a_high], axis=0).astype(bf16)
    out = dot(halves, b_high, dims, None)
    return out[:rows] + out[rows:] + dot(a_high.astype(bf16), b_low, dims, None)


def iota(shape, dim):
    return lax.broadcasted_iota(jnp.int32, shape, dim)


def each(count, body):
    if count <= UNROLL:
        for k in range(count):
            body(k)
    else:
        lax.fori_loop(0, count, lambda k, carry: (body(k), carry)[1], 0)


def total(ref, count, start):
    if count <= UNROLL:
        terms = [start] + [ref[k] for k in range(count)]
        while len(terms) > 1:
            terms = [sum(terms[i : i + 2][1:], terms[i]) for i in range(0, len(terms), 2)]
        return terms[0]
    return lax.fori_loop(0, count, lambda k, acc: acc + ref[k], start)


class Spread:
    def __init__(self, sizes, axes, source, slots, send, recv):
        self.sizes, self.axes = sizes, axes
        self.source, self.slots, self.send, self.recv = source, slots, send, recv
        self.count = peers_of(sizes, axes)

    def copy(self, k):
        return pltpu.make_async_remote_copy(
            src_ref=self.source,
            dst_ref=self.slots.at[k],
            send_sem=self.send.at[k],
            recv_sem=self.recv.at[k],
            device_id=peer(self.sizes, self.axes, k),
            device_id_type=MESH,
        )

    def start(self):
        each(self.count, lambda k: self.copy(k).start())

    def wait_recv(self):
        each(self.count, lambda k: self.copy(k).wait_recv())

    def wait_send(self):
        each(self.count, lambda k: self.copy(k).wait_send())


def peers_of(sizes, axes):
    clusters, members = sizes
    return {"both": clusters * members, "cluster": clusters, "sub": members}[axes] - 1


def peer(sizes, axes, k):
    clusters, members = sizes
    if axes == "both":
        c, m = (k + 1) // members, (k + 1) % members
        return {
            "cluster": lax.rem(lax.axis_index("cluster") + c, clusters),
            "sub": lax.rem(lax.axis_index("sub") + m, members),
        }
    count = clusters if axes == "cluster" else members
    return {axes: lax.rem(lax.axis_index(axes) + k + 1, count)}


def stages(sizes):
    return ("both",) if sizes[0] * sizes[1] <= UNROLL else ("cluster", "sub")


class AllSum:
    def __init__(self, sizes, refs, n):
        self.spreads = []
        for i, axes in enumerate(stages(sizes)):
            source, slots, send, recv = refs[4 * i : 4 * i + 4]
            self.spreads.append(
                Spread(sizes, axes, source.at[n], slots.at[n], send.at[n], recv.at[n])
            )

    def start(self):
        self.spreads[0].start()

    def finish(self):
        for i, spread in enumerate(self.spreads):
            spread.wait_recv()
            out = total(spread.slots, spread.count, spread.source[...])
            if i + 1 < len(self.spreads):
                self.spreads[i + 1].source[...] = out
                self.spreads[i + 1].start()
        return out

    def wait_send(self):
        for spread in self.spreads:
            spread.wait_send()


def kernel(sizes, *refs):
    clusters, members = sizes
    hbm, out_ref, refs = refs[:9], refs[9], list(refs[10:])

    def take_refs(count):
        taken = refs[:count]
        del refs[:count]
        return taken

    local_refs = take_refs(9)
    (
        rhs_ref,
        ops_ref,
        signs_ref,
        links_ref,
        cluster_basis_ref,
        corner_basis_ref,
        ids_ref,
        cluster_coarse_ref,
        global_coarse_ref,
    ) = local_refs
    (local_sem,) = take_refs(1)
    basis_ref, weights_ref, global_ref, picked_ref, swapped_basis_ref = take_refs(5)
    g_send, g_recv = take_refs(2)
    part_refs = take_refs(4)
    piece_slots, piece_send, piece_recv = take_refs(3)
    tail_refs = take_refs(4 * len(stages(sizes)))
    curve_refs = take_refs(4 * len(stages(sizes)))
    swap_refs = take_refs(8)
    table_refs = take_refs(8)

    subs, loads, dual = rhs_ref.shape
    rows = subs * loads
    kc, corn = cluster_basis_ref.shape[1], corner_basis_ref.shape[1]
    width = kc + corn
    coefs = subs * width
    order = global_coarse_ref.shape[1]
    solved = members * coefs
    my_c, my_s = lax.axis_index("cluster"), lax.axis_index("sub")
    has_low, has_high = my_s > 0, my_s < members - 1
    has_prev, has_next = my_c > 0, my_c < clusters - 1

    barrier = pltpu.get_barrier_semaphore()

    def greet(device_id):
        pl.semaphore_signal(barrier, inc=1, device_id=device_id, device_id_type=MESH)

    greeted = 0
    for axes in ("both",) if len(stages(sizes)) == 1 else ("cluster", "sub"):
        count = peers_of(sizes, axes)
        each(count, lambda k, axes=axes: greet(peer(sizes, axes, k)))
        greeted += count
    if len(stages(sizes)) > 1:
        for there, step in ((has_next, 1), (has_prev, -1)):

            @pl.when(there)
            def _():
                for m in range(1, members):
                    greet({"cluster": my_c + step, "sub": lax.rem(my_s + m, members)})

            greeted = greeted + there.astype(jnp.int32) * (members - 1)

    loads_in = [
        pltpu.make_async_copy(hbm[i], local_refs[i], local_sem.at[i]) for i in range(len(hbm))
    ]
    for i in (6, 5, 4, 0, 7, 8, 3, 2, 1):
        loads_in[i].start()
    numbers = iota((8, LANES), 1).astype(jnp.bfloat16)

    loads_in[6].wait()
    id_row = jnp.full((1, coefs), -1, jnp.int32)
    lane = iota((1, coefs), 1)
    for s in range(subs):
        for c in range(corn):
            id_row = jnp.where(lane == s * width + kc + c, ids_ref[s, c], id_row)
    id_col = jnp.sum(
        jnp.where(iota((coefs, coefs), 0) == iota((coefs, coefs), 1), id_row, 0),
        axis=1,
        keepdims=True,
    )
    weights_ref[:, solved:] = (id_col == iota((coefs, order), 1)).astype(jnp.float32)

    loads_in[5].wait()
    loads_in[4].wait()
    for s in range(subs):
        basis_ref[s * width : s * width + kc, :] = cluster_basis_ref[s]
        basis_ref[s * width + kc : (s + 1) * width, :] = corner_basis_ref[s]

    where_to = iota((1, solved), 1)
    within = lax.rem(where_to, width)
    source = (where_to // coefs) * (subs * kc) + (lax.rem(where_to, coefs) // width) * kc + within
    source = jnp.where(within < kc, source, -1)
    place = (iota((members * subs * kc, solved), 0) == source).astype(jnp.float32)
    loads_in[0].wait()
    loads_in[7].wait()
    coarse = dot(cluster_coarse_ref[0], place)
    for s in range(subs):
        weights_ref[s * width : s * width + kc, :solved] = coarse[s * kc : (s + 1) * kc]
        weights_ref[s * width + kc : (s + 1) * width, :solved] = jnp.zeros(
            (corn, solved), jnp.float32
        )

    diagonal = iota((rows, coefs), 0) // loads == iota((rows, coefs), 1) // width
    row_sub, lane_sub = iota((rows, coefs), 0) // loads, iota((rows, coefs), 1) // width
    crossed = row_sub + 1 - 2 * lax.rem(row_sub, 2) == lane_sub

    def per_load(x):
        out = x[:loads]
        for s in range(1, subs):
            out = out + x[s * loads : (s + 1) * loads]
        return out

    def lanes_added(x):
        out = x[:, :LANES]
        for b in range(1, dual // LANES):
            out = out + x[:, b * LANES : (b + 1) * LANES]
        return out

    def tiled(x):
        return jnp.concatenate([x] * subs, axis=0)

    lane_is_load = iota((loads, LANES), 0) == iota((loads, LANES), 1)

    def as_row(x):
        sums = jnp.sum(x, axis=1, keepdims=True)
        return jnp.sum(jnp.where(lane_is_load, sums, 0.0), axis=0, keepdims=True)

    def as_column(x):
        return jnp.sum(jnp.where(lane_is_load, x, 0.0), axis=1, keepdims=True)

    open_sends = []

    def piece_copy(n, side, k, step):
        target = lax.rem(my_s + k, members)
        return pltpu.make_async_remote_copy(
            src_ref=part_refs[0].at[n, target],
            dst_ref=piece_slots.at[n, side, k],
            send_sem=piece_send.at[n, side, k],
            recv_sem=piece_recv.at[n, side, k],
            device_id={"cluster": my_c + step, "sub": target},
            device_id_type=MESH,
        )

    def pieces(n, side, what):
        step = 1 - 2 * side
        for k in range(members):
            getattr(piece_copy(n, side, k, step), what)()

    def project_start(vector, n):
        raw = dot3(vector, basis_ref[...], NT)
        coef = per_load(jnp.where(diagonal, raw, 0.0))
        both = dot3(coef, weights_ref[...])
        tail_refs[0][n, :loads] = both[:, solved:]
        tail_refs[0][n, loads:, :LANES] = as_row(per_load(lanes_added(vector * vector)))
        if order > LANES:
            tail_refs[0][n, loads:, LANES:] = jnp.zeros((1, order - LANES), jnp.float32)
        for j in range(members):
            part_refs[0][n, j] = both[:, j * coefs : (j + 1) * coefs]
        tail = AllSum(sizes, tail_refs, n)
        tail.start()
        part = Spread(sizes, "sub", *[ref.at[n] for ref in part_refs])
        part.start()
        pl.when(has_next)(lambda: pieces(n, 0, "start"))
        pl.when(has_prev)(lambda: pieces(n, 1, "start"))
        return tail, part

    def project_finish(n, tail, part):
        part.wait_recv()
        pl.when(has_prev)(lambda: pieces(n, 0, "wait_recv"))
        pl.when(has_next)(lambda: pieces(n, 1, "wait_recv"))

        def cluster_of(member):
            out = part_refs[0][n, member]
            for k in range(members - 1):
                out = out + part_refs[1][n, k, member]
            return out

        def piece_sum(side):
            return total(piece_slots.at[n, side], members - 1, piece_slots[n, side, members - 1])

        own = cluster_of(my_s)
        high = cluster_of(jnp.minimum(my_s + 1, members - 1))
        low = cluster_of(jnp.maximum(my_s - 1, 0))
        prev, following = piece_sum(0), piece_sum(1)
        summed = tail.finish()
        open_sends.extend([tail, part])
        norm = as_column(summed[loads:, :LANES])
        corners = dot3(summed[:loads], picked_ref[...])

        def amount(base, i):
            return base + corners[:, i * coefs : (i + 1) * coefs]

        def block_diagonal(x, mask):
            return jnp.where(mask, tiled(x), 0.0)

        fix = dot3(block_diagonal(amount(own, 0), diagonal), basis_ref[...])
        high = jnp.where(has_high, amount(high, 1), 0.0)
        low = jnp.where(has_low, amount(low, 2), 0.0)
        following = jnp.where(has_next, amount(following, 3), 0.0)
        prev = jnp.where(has_prev, amount(prev, 4), 0.0)
        odd = lax.rem(iota((loads, coefs), 1) // width, 2) == 1
        cross = jnp.where(odd, following, prev)
        fix_swapped = jnp.concatenate(
            [
                dot3(block_diagonal(high, diagonal), swapped_basis_ref[0]),
                dot3(block_diagonal(low, diagonal), swapped_basis_ref[1]),
                dot3(block_diagonal(cross, crossed), swapped_basis_ref[2]),
            ],
            axis=1,
        )
        return fix, fix_swapped, norm

    def take(x, order_of):
        return jnp.take_along_axis(x, order_of, axis=1, mode="promise_in_bounds")

    class Swap:
        def __init__(self, refs, n):
            in_src, in_slots, in_send, in_recv, out_src, out_slots, out_send, out_recv = refs
            self.sources = [in_src.at[n, 0], in_src.at[n, 1], out_src.at[n, 0], out_src.at[n, 1]]
            self.slots = [
                in_slots.at[n, 0],
                in_slots.at[n, 1],
                out_slots.at[n, 0],
                out_slots.at[n, 1],
            ]
            self.send = [in_send.at[n, 0], in_send.at[n, 1], out_send.at[n, 0], out_send.at[n, 1]]
            self.recv = [in_recv.at[n, 0], in_recv.at[n, 1], out_recv.at[n, 0], out_recv.at[n, 1]]
            self.sends = [has_high, has_low, has_next, has_prev]
            self.takes = [has_low, has_high, has_prev, has_next]

        def copy(self, i):
            axis = "sub" if i < 2 else "cluster"
            return pltpu.make_async_remote_copy(
                src_ref=self.sources[i],
                dst_ref=self.slots[i],
                send_sem=self.send[i],
                recv_sem=self.recv[i],
                device_id={axis: lax.axis_index(axis) + (-1 if i % 2 else 1)},
                device_id_type=MESH,
            )

        def start(self, x, orders, height, extra=None):
            up_order, down_order, across_order = orders
            count = subs * height
            across = take(x[:, 2 * LANES :], across_order)
            for p in range(2):
                for h in range(subs // 2):
                    s = 2 * h + p
                    self.sources[2 + p][h * height : (h + 1) * height] = across[
                        s * height : (s + 1) * height
                    ]
            self.sources[0][:count] = take(x[:, :LANES], up_order)
            self.sources[1][:count] = take(x[:, LANES : 2 * LANES], down_order)
            if extra is not None:
                for i in range(4):
                    first = count if i < 2 else count // 2
                    self.sources[i][first : first + 8] = extra
            for i in (2, 3, 0, 1):
                pl.when(self.sends[i])(self.copy(i).start)

        def wait_recv(self):
            for i in range(4):
                pl.when(self.takes[i])(self.copy(i).wait_recv)

        def wait_send(self):
            for i in range(4):
                pl.when(self.sends[i])(self.copy(i).wait_send)

        def arrived(self, i):
            return jnp.where(self.takes[i], self.slots[i][...], 0.0)

        def field(self):
            self.wait_recv()
            at_odd, at_even = self.arrived(2), self.arrived(3)
            across = [
                (at_odd if s % 2 else at_even)[s // 2 * loads : (s // 2 + 1) * loads]
                for s in range(subs)
            ]
            return jnp.concatenate(
                [self.arrived(1), self.arrived(0), jnp.concatenate(across, axis=0)], axis=1
            )

    depth = global_coarse_ref.shape[0]
    own_rows = pl.ds(pl.multiple_of(my_s * depth, 8), depth)

    def gather_copy(k):
        return pltpu.make_async_remote_copy(
            src_ref=global_coarse_ref,
            dst_ref=global_ref.at[own_rows],
            send_sem=g_send.at[k],
            recv_sem=g_recv.at[k],
            device_id=peer(sizes, "sub", k),
            device_id_type=MESH,
        )

    def begin():
        loads_in[8].wait()
        global_ref[own_rows, :] = global_coarse_ref[...]
        each(members - 1, lambda k: gather_copy(k).start())
        loads_in[3].wait()

        def plain(row):
            return row

        def inverted(row):
            hot = (iota((LANES, LANES), 0) == row).astype(jnp.float32).astype(jnp.bfloat16)
            return dot(numbers, hot, NT, None)[:1].astype(jnp.int32)

        index = [
            [inverted(links_ref[0, s : s + 1, :]) for s in range(subs)],
            [plain(links_ref[1, s : s + 1, :]) for s in range(subs)],
            [(plain if s % 2 else inverted)(links_ref[2, s : s + 1, :]) for s in range(subs)],
        ]

        def orders_of(height):
            return [
                jnp.concatenate(
                    [jnp.broadcast_to(row, (height, LANES)) for row in block], axis=0
                )
                for block in index
            ]

        orders = orders_of(loads)
        rhs_swap = Swap(swap_refs, ITERS)
        rhs_swap.start(rhs, orders, loads)
        tables = Swap(table_refs, 0)
        ids_sent = jnp.broadcast_to(id_row.astype(jnp.float32), (8, coefs))
        tables.start(basis_ref[...], orders_of(width), width, ids_sent)

        loads_in[2].wait()
        sign = jnp.concatenate(
            [
                jnp.broadcast_to(signs_ref[s : s + 1, :].astype(jnp.float32), (loads, dual))
                for s in range(subs)
            ],
            axis=0,
        )
        each(members - 1, lambda k: gather_copy(k).wait_recv())
        tables.wait_recv()
        swapped_basis_ref[0] = tables.arrived(1)[:coefs]
        swapped_basis_ref[1] = tables.arrived(0)[:coefs]
        from_prev, from_next = tables.arrived(2), tables.arrived(3)
        for s in range(subs):
            swapped_basis_ref[2, s * width : (s + 1) * width] = (
                from_next if s % 2 else from_prev
            )[s // 2 * width : (s // 2 + 1) * width]
        id_rows = [id_row.astype(jnp.float32)]
        for i in (1, 0, 3, 2):
            first = coefs if i < 2 else coefs // 2
            id_rows.append(tables.slots[i][first : first + 1])
        whose = iota((order, coefs), 0).astype(jnp.float32)
        picks = jnp.concatenate([(row == whose).astype(jnp.float32) for row in id_rows], axis=1)
        for r in range(0, order, 2 * LANES):
            chunk = slice(r, min(r + 2 * LANES, order))
            picked_ref[chunk] = dot(global_ref[chunk], picks)
        loads_in[1].wait()
        open_sends.extend([rhs_swap, tables])
        return sign, orders, rhs_swap.field()

    rhs = jnp.concatenate([rhs_ref[s] for s in range(subs)], axis=0)
    pl.semaphore_wait(barrier, greeted)
    started = project_start(rhs, 0)
    sign, orders, residual_swapped = begin()
    fix, fix_swapped, rho = project_finish(0, *started)
    residual = rhs
    direction, direction_swapped = residual - fix, residual_swapped - fix_swapped
    row_odd = lax.rem(iota((rows, LANES), 0) // loads, 2) == 1
    there = jnp.concatenate(
        [
            jnp.full((rows, LANES), has_high.astype(jnp.float32)),
            jnp.full((rows, LANES), has_low.astype(jnp.float32)),
            jnp.where(row_odd, has_prev.astype(jnp.float32), has_next.astype(jnp.float32)),
        ],
        axis=1,
    )
    multipliers = None
    for n in range(ITERS):
        spread = sign * (direction + direction_swapped)
        spread_bf = spread.astype(jnp.bfloat16)
        image = jnp.concatenate(
            [
                dot(spread_bf[s * loads : (s + 1) * loads], ops_ref[s], NN, None)
                for s in range(subs)
            ],
            axis=0,
        )
        curve_refs[0][n] = as_row(per_load(lanes_added(spread * image)))
        curve = AllSum(sizes, curve_refs, n)
        curve.start()
        signed = sign * image
        swap = Swap(swap_refs, n)
        swap.start(signed, orders, loads)
        signed_swapped = swap.field()
        product = signed + signed_swapped
        product_swapped = signed_swapped + there * signed
        curvature = as_column(curve.finish())
        open_sends.extend([curve, swap])
        step = tiled(rho / curvature)
        residual = residual - step * product
        if n + 1 < ITERS:
            started = project_start(residual, n + 1)
        moved = step * direction
        multipliers = moved if multipliers is None else multipliers + moved
        if n + 1 < ITERS:
            residual_swapped = residual_swapped - step * product_swapped
            fix, fix_swapped, rho_new = project_finish(n + 1, *started)
            ratio = tiled(rho_new / rho)
            direction = residual - fix + ratio * direction
            direction_swapped = residual_swapped - fix_swapped + ratio * direction_swapped
            rho = rho_new
    for s in range(subs):
        out_ref[0, s] = multipliers[s * loads : (s + 1) * loads]
        out_ref[1, s] = residual[s * loads : (s + 1) * loads]
    for spread in open_sends:
        spread.wait_send()
    each(members - 1, lambda k: gather_copy(k).wait_send())
    for n in range(ITERS):
        pl.when(has_next)(lambda n=n: pieces(n, 0, "wait_send"))
        pl.when(has_prev)(lambda n=n: pieces(n, 1, "wait_send"))


def split(both_ref, mult_ref, res_ref):
    mult_ref[...] = both_ref[0]
    res_ref[...] = both_ref[1]


def local(sizes, *args):
    args = list(args)
    args[3] = jnp.transpose(args[3], (1, 0, 2))
    rhs, operators, signs, links, cluster_basis, corner_basis, ids, coarse, glob = args
    clusters, members = sizes
    subs, loads, dual = rhs.shape
    coefs = subs * (cluster_basis.shape[1] + corner_basis.shape[1])
    depth, order = glob.shape
    f32 = jnp.float32
    dma = pltpu.SemaphoreType.DMA

    def exchange(lead, block, receive):
        return [
            pltpu.VMEM(lead[:1] + block, f32),
            pltpu.VMEM(lead + receive, f32),
            dma(lead),
            dma(lead),
        ]

    def swap_scratch(count, height, extra):
        scratch = []
        for rows in (subs * height + extra, subs * height // 2 + extra):
            scratch += [
                pltpu.VMEM((count, 2, rows, LANES), f32),
                pltpu.VMEM((count, 2, rows, LANES), f32),
                dma((count, 2)),
                dma((count, 2)),
            ]
        return scratch

    def sum_scratch(block):
        scratch = []
        for axes in stages(sizes):
            scratch += exchange((ITERS, peers_of(sizes, axes)), block, block)
        return scratch

    vmem = pl.BlockSpec(memory_space=pltpu.VMEM)
    scratch = [pltpu.VMEM(a.shape, a.dtype) for a in args]
    scratch[6] = pltpu.SMEM(ids.shape, ids.dtype)
    scratch += [
        dma((len(args),)),
        pltpu.VMEM((coefs, dual), f32),
        pltpu.VMEM((coefs, members * coefs + order), f32),
        pltpu.VMEM((order, order), f32),
        pltpu.VMEM((order, 5 * coefs), f32),
        pltpu.VMEM((3, coefs, LANES), f32),
        dma((members - 1,)),
        dma((members - 1,)),
    ]
    part = (members, loads, coefs)
    scratch += exchange((ITERS, members - 1), part, part)
    scratch += [
        pltpu.VMEM((ITERS, 2, members, loads, coefs), f32),
        dma((ITERS, 2, members)),
        dma((ITERS, 2, members)),
    ]
    scratch += sum_scratch((loads + 1, order)) + sum_scratch((1, LANES))
    scratch += swap_scratch(ITERS + 1, loads, 0)
    scratch += swap_scratch(1, coefs // subs, 8)
    both = pl.pallas_call(
        functools.partial(kernel, sizes),
        out_shape=jax.ShapeDtypeStruct((2,) + rhs.shape, f32),
        in_specs=[pl.BlockSpec(memory_space=pl.ANY)] * len(args),
        out_specs=vmem,
        scratch_shapes=scratch,
        compiler_params=pltpu.CompilerParams(collective_id=0, has_side_effects=True),
    )(*args)
    return pl.pallas_call(
        split,
        out_shape=[jax.ShapeDtypeStruct(rhs.shape, f32)] * 2,
        in_specs=[vmem],
        out_specs=[vmem, vmem],
    )(both)


def solution(mesh):
    placed = (
        P(("cluster", "sub"), None, None),
        P(("cluster", "sub"), None, None),
        P(("cluster", "sub"), None),
        P(("cluster", "sub"), None, None),
        P(("cluster", "sub"), None, None),
        P(("cluster", "sub"), None, None),
        P(("cluster", "sub"), None),
        P("cluster", "sub", None),
        P("sub", None),
    )
    return jax.shard_map(
        functools.partial(local, (mesh.shape["cluster"], mesh.shape["sub"])),
        mesh=mesh,
        in_specs=placed,
        out_specs=(P(("cluster", "sub"), None, None), P(("cluster", "sub"), None, None)),
        check_vma=False,
    )
```
